128 devices in a mesh: tm: 32 (over y, z, core), node: 4 (over x).
Axes of the slice: x: 4, y: 4, z: 4, core: 2. Of those that a mesh axis runs over, the one named last changes fastest.
Arguments:
- slice_starts: float32 [32, 32, 16384], P('tm'), may hold values from -1 to 1
- coupling: float32 [32, 16384], replicated, may hold values from 0.03 to 0.25
Outputs:
- node_values: float32 [32, 4, 32, 16384], P('tm', 'node')
- residual_log: float32 [3, 32], replicated
The draws below stay inside these ranges and needn't reach their ends.
All inputs are finite; a program needn't handle non-finite values.
Results may differ from the reference program's by a relative error of at most 0.0001.
Values sent between devices are 32-bit elements.
A program may use at most 128 MiB of HBM per device.

```python
import math
import jax
import jax.numpy as jnp
from jax import lax

X = 16384
SYS = 32
M = 4
SWEEPS = 3
NEWTON = 2
SLICES = 32


def block_scale(stream_key, shape, pieces, least, top_value):
    level, own = 1.0, jax.random.fold_in(stream_key, 6)
    for position, shards_of in pieces:
        draws = jnp.exp(jax.random.uniform(jax.random.fold_in(own, position), (shards_of,), jnp.float32, least / len(pieces), top_value / len(pieces)))
        level = level * jnp.repeat(draws, shape[position] // shards_of).reshape([-1 if axis == position else 1 for axis in range(len(shape))])
    return level


def setup_inputs(seed: int = 0) -> dict:
    key_of = jax.random.split(jax.random.key(seed), 3)
    return {
        "slice_starts": jnp.clip(jax.random.uniform(key_of[0], (SLICES, SYS, X), jnp.float32, -1.0, 1.0) * block_scale(key_of[0], (SLICES, SYS, X), ((0, 32),), -0.4, 0.0), -1.0, 1.0),
        "coupling": jnp.clip(jnp.exp(jax.random.uniform(key_of[1], (SYS, X), jnp.float32, math.log(0.03), math.log(0.25))), 0.03, 0.25),
    }


time_step = 0.5
log_floor = 0.05


def legendre_gap(point, node_count):
    before = 1.0
    current = point
    for degree in range(1, node_count):
        following = ((2 * degree + 1) * point * current - degree * before) / (degree + 1)
        before = current
        current = following
    return current - before


def collocation(node_count):
    points = []
    samples = 4000
    for sample_index in range(samples - 1):
        lower_end = -1.0 + 2.0 * sample_index / samples
        upper_end = -1.0 + 2.0 * (sample_index + 1) / samples
        lower_value = legendre_gap(lower_end, node_count)
        upper_value = legendre_gap(upper_end, node_count)
        if lower_value * upper_value < 0.0:
            for halving in range(80):
                middle = 0.5 * (lower_end + upper_end)
                middle_value = legendre_gap(middle, node_count)
                if lower_value * middle_value <= 0.0:
                    upper_end = middle
                else:
                    lower_end = middle
                    lower_value = middle_value
            points.append(0.5 * (lower_end + upper_end))
    points.append(1.0)
    node_times = [(point + 1.0) / 2.0 for point in points]
    matrix = [[0.0] * node_count for row_index in range(node_count)]
    for column in range(node_count):
        coeffs = [1.0]
        for other in range(node_count):
            if other != column:
                scale = node_times[column] - node_times[other]
                shifted = [0.0] + coeffs
                scaled = [value * node_times[other] for value in coeffs] + [0.0]
                coeffs = [(shifted[power] - scaled[power]) / scale for power in range(len(shifted))]
        for row_index in range(node_count):
            upper_time = node_times[row_index]
            matrix[row_index][column] = sum(coeffs[power] * upper_time ** (power + 1) / (power + 1) for power in range(len(coeffs)))
    return node_times, matrix


def operator_term(field_values, coupling):
    right_side = jnp.roll(field_values, -1, axis=-1)
    left_side = jnp.roll(field_values, 1, axis=-1)
    left_coupling = jnp.roll(coupling, 1, axis=-1)
    cubic = field_values * field_values * field_values
    return coupling * (right_side - field_values) - left_coupling * (field_values - left_side) + field_values - cubic


def reference(slice_starts, coupling):
    node_times, matrix = collocation(M)
    weights = jnp.asarray(matrix, jnp.float32)
    diag_weights = jnp.asarray([time_step * moment / M for moment in node_times], jnp.float32)
    implicit = diag_weights[None, :, None, None]
    node_state = jnp.broadcast_to(slice_starts[:, None], (SLICES, M, SYS, X))
    end_values = slice_starts
    residual_list = []
    for sweep_index in range(SWEEPS):
        starts = jnp.concatenate([slice_starts[:1], end_values[:-1]], axis=0)
        forcing = operator_term(node_state, coupling)
        quadrature = jnp.einsum("mj,pjsx->pmsx", weights, forcing, precision=lax.Precision.HIGHEST)
        base = starts[:, None] + time_step * quadrature
        defect = base - node_state
        mean_square = jnp.sum(defect * defect, axis=(0, 1, 3)) / (SLICES * M * X)
        residual_list.append(jnp.log(log_floor + mean_square))
        target = base - implicit * (node_state - node_state * node_state * node_state)
        iterate = node_state
        for newton_step in range(NEWTON):
            cubic = iterate * iterate * iterate
            derivative = 1.0 - implicit + 3.0 * implicit * iterate * iterate
            iterate = iterate - (iterate - implicit * (iterate - cubic) - target) / derivative
        node_state = iterate
        end_values = node_state[:, M - 1]
    return node_state, jnp.stack(residual_list)
```

```python
import functools

import jax
import jax.numpy as jnp
import numpy as np
from jax import lax
from jax.experimental import pallas as pl
from jax.experimental.pallas import tpu as pltpu
from jax.sharding import PartitionSpec as P

M = 4
SWEEPS = 3
CORES = 2
LANES = 128
ROWS = 8
TILE = 4
PAD = 5
time_step = 0.5
log_floor = 0.05


def legendre_gap(point, node_count):
    before = 1.0
    current = point
    for degree in range(1, node_count):
        following = ((2 * degree + 1) * point * current - degree * before) / (degree + 1)
        before = current
        current = following
    return current - before


def collocation(node_count):
    points = []
    samples = 4000
    for sample_index in range(samples - 1):
        lower_end = -1.0 + 2.0 * sample_index / samples
        upper_end = -1.0 + 2.0 * (sample_index + 1) / samples
        lower_value = legendre_gap(lower_end, node_count)
        upper_value = legendre_gap(upper_end, node_count)
        if lower_value * upper_value < 0.0:
            for halving in range(80):
                middle = 0.5 * (lower_end + upper_end)
                middle_value = legendre_gap(middle, node_count)
                if lower_value * middle_value <= 0.0:
                    upper_end = middle
                else:
                    lower_end = middle
                    lower_value = middle_value
            points.append(0.5 * (lower_end + upper_end))
    points.append(1.0)
    node_times = [(point + 1.0) / 2.0 for point in points]
    matrix = [[0.0] * node_count for row_index in range(node_count)]
    for column in range(node_count):
        coeffs = [1.0]
        for other in range(node_count):
            if other != column:
                scale = node_times[column] - node_times[other]
                shifted = [0.0] + coeffs
                scaled = [value * node_times[other] for value in coeffs] + [0.0]
                coeffs = [(shifted[power] - scaled[power]) / scale for power in range(len(shifted))]
        for row_index in range(node_count):
            upper_time = node_times[row_index]
            matrix[row_index][column] = sum(
                coeffs[power] * upper_time ** (power + 1) / (power + 1) for power in range(len(coeffs))
            )
    return (node_times, matrix)


NODE_TIMES, MATRIX = collocation(M)
WEIGHTS = [[time_step * float(np.float32(q)) for q in row] for row in MATRIX]
IMPLICIT = [float(np.float32(time_step * t / M)) for t in NODE_TIMES]
ROW_SUMS = [sum(row) for row in WEIGHTS]


def kernel(sizes, ss_ref, cp_ref, out_ref, res_ref, buf, cbuf, u1, e1, u2, e2, rbuf, acc, st1, st2, st3,
           csem, rsem, zsend, osend, orecv, s1s, s1r, s2s, s2r, s3s, s3r):
    ny, nz, cells, mean_count = sizes
    half = cells // LANES // CORES
    tiles = half // TILE
    whole = cells // LANES
    chips = ny * nz
    tm = lax.axis_index("tm")
    node = lax.axis_index("node")
    core = lax.rem(tm, CORES)
    chip = lax.div(tm, CORES)
    zpos = lax.rem(chip, nz)
    ypos = lax.div(chip, nz)
    rows = pl.ds(pl.multiple_of(node * ROWS, ROWS), ROWS)

    def at_chip(by, which):
        return lax.rem(chip + by + 2 * chips, chips) * CORES + which

    def at_zcore(slot):
        return ypos * (nz * CORES) + slot

    def at_y(slot):
        return slot * (nz * CORES) + lax.rem(tm, nz * CORES)

    def cols(start, count):
        if isinstance(start, int):
            return pl.ds(start * LANES, count * LANES)
        return pl.ds(pl.multiple_of(start * LANES, LANES), count * LANES)

    def remote(src, dst, send, recv, to_tm, to_node):
        return pltpu.make_async_remote_copy(
            src, dst, send, recv, device_id=(to_tm, to_node), device_id_type=pl.DeviceIdType.MESH
        )

    def source(which, a):
        if isinstance(a, int) and a == 0:
            return lax.rem(half * which + whole - 1, whole), PAD - 1, 1
        return lax.rem(half * which + TILE * (a - 1), whole), PAD + TILE * (a - 1), TILE

    def local_set(a):
        start, q, count = source(core, a)
        pltpu.make_async_copy(cp_ref.at[rows, cols(start, count)], cbuf.at[:, cols(q, count)], csem.at[a]).start()
        pltpu.make_async_copy(
            ss_ref.at[0, rows, cols(start, count)], buf.at[3 + core, :, cols(q, count)], rsem.at[3 + core, a]
        ).start()

    def remote_set(a):
        @pl.when(core == 1)
        def _():
            for which in range(CORES):
                start, q, count = source(which, a)
                remote(ss_ref.at[0, rows, cols(start, count)], buf.at[0, :, cols(q, count)],
                       zsend.at[2 + which], rsem.at[0, a], at_chip(2, which), node).start()

        for which in range(CORES):
            start, q, count = source(which, a)
            remote(ss_ref.at[0, rows, cols(start, count)], buf.at[1 + core, :, cols(q, count)],
                   zsend.at[which], rsem.at[1 + core, a], at_chip(1, which), node).start()
        start, q, count = source(1 - core, a)
        remote(ss_ref.at[0, rows, cols(start, count)], buf.at[3 + core, :, cols(q, count)],
               zsend.at[4], rsem.at[3 + core, a], at_chip(0, 1 - core), node).start()

    def wait_set(a):
        _, q, count = source(core, a)
        pltpu.make_async_copy(cbuf.at[:, cols(q, count)], cbuf.at[:, cols(q, count)], csem.at[a]).wait()
        for n in range(5):
            view = buf.at[n, :, cols(q, count)]
            pltpu.make_async_copy(view, view, rsem.at[n, a]).wait()

    local_set(0)

    @pl.loop(1, tiles + 2)
    def _(a):
        local_set(a)

    barrier = pltpu.get_barrier_semaphore()
    greeted = 0

    def greet(to_tm, to_node):
        pl.semaphore_signal(barrier, inc=1, device_id=(to_tm, to_node), device_id_type=pl.DeviceIdType.MESH)

    greet(at_chip(0, 1 - core), node)
    greeted += 1
    for by in range(1, M):
        for which in range(CORES):
            greet(at_chip(0, which), lax.rem(node + by, M))
            greeted += 1
    for by in (1, 2, -1, -2):
        for which in range(CORES):
            greet(at_chip(by, which), node)
            greeted += 1
    for by in range(1, nz):
        for which in range(CORES):
            greet(at_zcore(lax.rem(zpos + by, nz) * CORES + which), node)
            greeted += 1
    for by in range(1, ny):
        greet(at_y(lax.rem(ypos + by, ny)), node)
        greeted += 1
    pl.semaphore_wait(barrier, greeted)

    remote_set(0)

    @pl.loop(1, tiles + 2)
    def _(a):
        remote_set(a)

    acc[...] = jnp.zeros_like(acc)
    first = chip == 0
    second = chip == 1
    width = TILE * LANES

    def force(ref, q, cw):
        x = ref[:, cols(q - 1, TILE + 2)]
        flux = cw * (pltpu.roll(x, (TILE + 2) * LANES - 1, axis=1) - x)
        spread = flux - pltpu.roll(flux, 1, axis=1)
        u = x[:, LANES:LANES + width]
        square = u * u
        g = u - u * square
        return u, square, g, spread[:, LANES:LANES + width] + g

    def newton(u, square, g, base, m):
        a = IMPLICIT[m]
        defect = base - u
        target = base - a * g
        once = u + defect / ((1.0 - a) + (3.0 * a) * square)
        square = once * once
        twice = (target + (2.0 * a) * square * once) / ((1.0 - a) + (3.0 * a) * square)
        return twice, defect

    def add_up(k, q, total):
        parts = []
        for t in range(TILE):
            mine = jnp.logical_and(q + t >= PAD, q + t < PAD + half)
            part = total[:, t * LANES:(t + 1) * LANES]
            parts.append(jnp.where(mine, part, jnp.zeros_like(part)))
        acc[k] += (parts[0] + parts[1]) + (parts[2] + parts[3])

    def start_sweep(q):
        cw = cbuf[:, cols(q - 1, TILE + 2)]
        here = cols(q, TILE)
        total = None
        for n in range(1, 5):
            u, square, g, f = force(buf.at[n], q, cw)
            before = buf[n - 1, :, here]
            if n == 3:
                before = jnp.where(first, u, before)
            if n == 1:
                before = jnp.where(second, u, before)
            for m in range(M):
                if n == 1 and m < M - 1:
                    continue
                new, defect = newton(u, square, g, before + ROW_SUMS[m] * f, m)
                if n == 1:
                    e1[:, here] = new
                else:
                    u1[n - 2, m, :, here] = new
                if n >= 3:
                    total = defect * defect if total is None else total + defect * defect
        add_up(0, q, total)

    def later_sweep(k, q):
        cw = cbuf[:, cols(q - 1, TILE + 2)]
        here = cols(q, TILE)
        total = None
        old = u1 if k == 1 else u2
        for n in range(2 if k == 1 else 3, 5):
            slot = n - 2 if k == 1 else n - 3
            parts = [force(old.at[slot, m], q, cw) for m in range(M)]
            if n == 2:
                before = e1[:, here]
            elif n == 3:
                before = u1[0, M - 1, :, here] if k == 1 else e2[:, here]
                before = jnp.where(first, buf[3, :, here], before)
            else:
                before = old[slot - 1, M - 1, :, here]
            for m in range(M):
                if n == 2 and m < M - 1:
                    continue
                base = before
                for j in range(M):
                    base = base + WEIGHTS[m][j] * parts[j][3]
                new, defect = newton(parts[m][0], parts[m][1], parts[m][2], base, m)
                if n == 2:
                    e2[:, here] = new
                elif k == 1:
                    u2[n - 3, m, :, here] = new
                else:
                    rbuf[n - 3, m, :, here] = new
                if n >= 3:
                    total = defect * defect if total is None else total + defect * defect
        add_up(k, q, total)

    def send_out(i):
        q = PAD + TILE * i
        place = cols(core * half + TILE * i, TILE)
        for away in range(M):
            to_node = lax.rem(node + away, M)
            for other in range(CORES):
                which = core if other == 0 else 1 - core
                src = rbuf.at[which, to_node, :, cols(q, TILE)]
                dst = out_ref.at[0, 0, rows, place]
                if away == 0 and other == 0:
                    pltpu.make_async_copy(src, dst, osend.at[0, 0]).start()
                else:
                    remote(src, dst, osend.at[other, away], orecv.at[other, away],
                           at_chip(0, which), to_node).start()

    wait_set(0)

    @pl.loop(0, tiles + 1)
    def _(step):
        i = step - 1
        wait_set(step + 1)
        q = PAD + TILE * i
        start_sweep(q + 2)
        later_sweep(1, q + 1)
        later_sweep(2, q)

        @pl.when(step > 0)
        def _():
            send_out(i)

    lane = lax.broadcasted_iota(jnp.int32, (ROWS, LANES), 1)
    sums = jnp.zeros((ROWS, LANES), jnp.float32)
    for k in range(SWEEPS):
        sums = jnp.where(lane == k, jnp.sum(acc[k], axis=1, keepdims=True), sums)
    zcore = lax.rem(tm, nz * CORES)
    st1[zcore] = sums
    flows = []
    for by in range(1, nz * CORES):
        to = at_zcore(lax.rem(zcore + by, nz * CORES))
        c = remote(st1.at[zcore], st1.at[zcore], s1s.at[by], s1r.at[by], to, node)
        c.start()
        flows.append(c)
    for c in flows:
        c.wait()
    sums = st1[0]
    for slot in range(1, nz * CORES):
        sums = sums + st1[slot]
    st2[ypos] = sums
    flows = []
    for by in range(1, ny):
        c = remote(st2.at[ypos], st2.at[ypos], s2s.at[by], s2r.at[by], at_y(lax.rem(ypos + by, ny)), node)
        c.start()
        flows.append(c)
    for c in flows:
        c.wait()
    sums = st2[0]
    for slot in range(1, ny):
        sums = sums + st2[slot]
    st3[node] = sums
    flows = []
    for by in range(1, M):
        c = remote(st3.at[node], st3.at[node], s3s.at[by], s3r.at[by], tm, lax.rem(node + by, M))
        c.start()
        flows.append(c)
    for c in flows:
        c.wait()
    table = jnp.concatenate([st3[m] for m in range(M)] + [jnp.zeros((LANES - M * ROWS, LANES), jnp.float32)], axis=0)
    table = jnp.log(log_floor + table.T / mean_count)
    res_ref[...] = table[:SWEEPS, :M * ROWS]

    sent = buf.at[0, :, cols(0, 1 + TILE * (tiles + 1))]
    for flow in (0, 1, 4):
        pltpu.make_async_copy(sent, sent, zsend.at[flow]).wait()

    @pl.when(core == 1)
    def _():
        for flow in (2, 3):
            pltpu.make_async_copy(sent, sent, zsend.at[flow]).wait()

    made = rbuf.at[0, 0, :, cols(0, half)]
    for away in range(M):
        for other in range(CORES):
            pltpu.make_async_copy(made, made, osend.at[other, away]).wait()
            if away or other:
                pltpu.make_async_copy(made, made, orecv.at[other, away]).wait()


def body(sizes, slice_starts, coupling):
    systems, cells = coupling.shape
    ny, nz = sizes
    half = cells // LANES // CORES
    tiles = half // TILE
    span = half + PAD + TILE
    mean_count = float(ny * nz * CORES * M * cells)
    flat = lambda *lead: pltpu.VMEM(lead + (ROWS, span * LANES), jnp.float32)
    dma = pltpu.SemaphoreType.DMA
    any_spec = pl.BlockSpec(memory_space=pl.ANY)
    return pl.pallas_call(
        functools.partial(kernel, (ny, nz, cells, mean_count)),
        out_shape=(
            jax.ShapeDtypeStruct((1, 1, systems, cells), jnp.float32),
            jax.ShapeDtypeStruct((SWEEPS, systems), jnp.float32),
        ),
        in_specs=[any_spec, any_spec],
        out_specs=(any_spec, pl.BlockSpec(memory_space=pltpu.VMEM)),
        scratch_shapes=[
            flat(5), flat(), flat(3, M), flat(), flat(2, M), flat(), flat(2, M),
            pltpu.VMEM((SWEEPS, ROWS, LANES), jnp.float32),
            pltpu.VMEM((nz * CORES, ROWS, LANES), jnp.float32),
            pltpu.VMEM((ny, ROWS, LANES), jnp.float32),
            pltpu.VMEM((M, ROWS, LANES), jnp.float32),
            dma((tiles + 2,)), dma((5, tiles + 2)), dma((5,)), dma((CORES, M)), dma((CORES, M)),
            dma((nz * CORES,)), dma((nz * CORES,)), dma((ny,)), dma((ny,)), dma((M,)), dma((M,)),
        ],
        compiler_params=pltpu.CompilerParams(
            collective_id=0, has_side_effects=True, vmem_limit_bytes=48 * 2**20
        ),
        name="sdc",
    )(slice_starts, coupling)


def solution(mesh):
    chips = mesh.shape["tm"] // CORES
    ny = 4
    return jax.shard_map(
        functools.partial(body, (ny, chips // ny)),
        mesh=mesh,
        in_specs=(P("tm", None, None), P()),
        out_specs=(P("tm", "node", None, None), P()),
        check_vma=False,
    )
```

```python
import functools

import jax
import jax.numpy as jnp
import numpy as np
from jax import lax
from jax.experimental import pallas as pl
from jax.experimental.pallas import tpu as pltpu
from jax.sharding import PartitionSpec as P

M = 4
SWEEPS = 3
CORES = 2
LANES = 128
ROWS = 8
TILE = 4
PAD = 5
time_step = 0.5
log_floor = 0.05


def legendre_gap(point, node_count):
    before = 1.0
    current = point
    for degree in range(1, node_count):
        following = ((2 * degree + 1) * point * current - degree * before) / (degree + 1)
        before = current
        current = following
    return current - before


def collocation(node_count):
    points = []
    samples = 4000
    for sample_index in range(samples - 1):
        lower_end = -1.0 + 2.0 * sample_index / samples
        upper_end = -1.0 + 2.0 * (sample_index + 1) / samples
        lower_value = legendre_gap(lower_end, node_count)
        upper_value = legendre_gap(upper_end, node_count)
        if lower_value * upper_value < 0.0:
            for halving in range(80):
                middle = 0.5 * (lower_end + upper_end)
                middle_value = legendre_gap(middle, node_count)
                if lower_value * middle_value <= 0.0:
                    upper_end = middle
                else:
                    lower_end = middle
                    lower_value = middle_value
            points.append(0.5 * (lower_end + upper_end))
    points.append(1.0)
    node_times = [(point + 1.0) / 2.0 for point in points]
    matrix = [[0.0] * node_count for row_index in range(node_count)]
    for column in range(node_count):
        coeffs = [1.0]
        for other in range(node_count):
            if other != column:
                scale = node_times[column] - node_times[other]
                shifted = [0.0] + coeffs
                scaled = [value * node_times[other] for value in coeffs] + [0.0]
                coeffs = [(shifted[power] - scaled[power]) / scale for power in range(len(shifted))]
        for row_index in range(node_count):
            upper_time = node_times[row_index]
            matrix[row_index][column] = sum(
                coeffs[power] * upper_time ** (power + 1) / (power + 1) for power in range(len(coeffs))
            )
    return (node_times, matrix)


NODE_TIMES, MATRIX = collocation(M)
WEIGHTS = [[time_step * float(np.float32(q)) for q in row] for row in MATRIX]
IMPLICIT = [float(np.float32(time_step * t / M)) for t in NODE_TIMES]
ROW_SUMS = [sum(row) for row in WEIGHTS]


DIRECT = 5
LEAD = 5


def kernel(sizes, ss_ref, cp_ref, out_ref, res_ref, own, transit, buf, cbuf, u1, e1, u2, e2, rbuf, acc, st1, st2, st3,
           wsem, csem, rsem, tsem, zsend, osend, orecv, s1s, s1r, s2s, s2r, s3s, s3r):
    ny, nz, cells, mean_count = sizes
    half = cells // LANES // CORES
    tiles = half // TILE
    whole = cells // LANES
    chips = ny * nz
    sets = tiles + 2
    tm = lax.axis_index("tm")
    node = lax.axis_index("node")
    core = lax.rem(tm, CORES)
    chip = lax.div(tm, CORES)
    zpos = lax.rem(chip, nz)
    ypos = lax.div(chip, nz)
    rows = pl.ds(pl.multiple_of(node * ROWS, ROWS), ROWS)

    middle = jnp.where(zpos == 0, chip + nz - 1, chip - 1)
    source_chip = jnp.where(zpos == nz - 1, chip - nz + 1, chip + 1)
    target = jnp.where(zpos == nz - 1, chip - 1, chip + nz - 1)
    middle_of_target = jnp.where(zpos == 2, chip + 1, chip - nz + 1)
    has_next = chip < chips - 1
    has_before = chip > 0
    far_source = jnp.logical_and(core == 1, chip < chips - 2)
    far_target = chip > 1
    is_middle = source_chip < chips - 2
    far_middle = jnp.logical_and(core == 0, is_middle)

    def dev(which_chip, which):
        return which_chip * CORES + which

    def cols(start, count):
        if isinstance(start, int):
            return pl.ds(start * LANES, count * LANES)
        return pl.ds(pl.multiple_of(start * LANES, LANES), count * LANES)

    def remote(src, dst, send, recv, to_tm, to_node):
        return pltpu.make_async_remote_copy(
            src, dst, send, recv, device_id=(to_tm, to_node), device_id_type=pl.DeviceIdType.MESH
        )

    def source(which, a):
        if isinstance(a, int) and a == 0:
            return lax.rem(half * which + whole - 1, whole), PAD - 1, 1
        return lax.rem(half * which + TILE * (a - 1), whole), PAD + TILE * (a - 1), TILE

    def local_set(a):
        start, q, count = source(core, a)
        pltpu.make_async_copy(cp_ref.at[rows, cols(start, count)], cbuf.at[:, cols(q, count)], csem.at[a]).start()
        pltpu.make_async_copy(
            ss_ref.at[0, rows, cols(start, count)], buf.at[3 + core, :, cols(q, count)], rsem.at[3 + core, a]
        ).start()

    def near_set(a):
        @pl.when(has_next)
        def _():
            for which in range(CORES):
                start, q, count = source(which, a)
                remote(own.at[:, cols(start, count)], buf.at[1 + core, :, cols(q, count)],
                       zsend.at[which], rsem.at[1 + core, a], dev(chip + 1, which), node).start()

        start, q, count = source(1 - core, a)
        remote(own.at[:, cols(start, count)], buf.at[3 + core, :, cols(q, count)],
               zsend.at[4], rsem.at[3 + core, a], dev(chip, 1 - core), node).start()

    def direct_set(a):
        @pl.when(far_source)
        def _():
            for which in range(CORES):
                start, q, count = source(which, a)
                remote(own.at[:, cols(start, count)], buf.at[0, :, cols(q, count)],
                       zsend.at[2 + which], rsem.at[0, a], dev(chip + 2, which), node).start()

    def first_leg(a):
        @pl.when(far_source)
        def _():
            for which in range(CORES):
                start, q, count = source(which, a)
                remote(own.at[:, cols(start, count)], transit.at[which, :, cols(q, count)],
                       zsend.at[5 + which], tsem.at[which, a], dev(middle, 0), node).start()

    def second_leg(a):
        for which in range(CORES):
            _, q, count = source(which, a)
            view = transit.at[which, :, cols(q, count)]
            pltpu.make_async_copy(view, view, tsem.at[which, a]).wait()
            remote(view, buf.at[0, :, cols(q, count)],
                   zsend.at[7 + which], rsem.at[0, a], dev(target, which), node).start()

    def wait_set(a):
        _, q, count = source(core, a)
        pltpu.make_async_copy(cbuf.at[:, cols(q, count)], cbuf.at[:, cols(q, count)], csem.at[a]).wait()

        def arrived(n):
            view = buf.at[n, :, cols(q, count)]
            pltpu.make_async_copy(view, view, rsem.at[n, a]).wait()

        arrived(3)
        arrived(4)

        @pl.when(has_before)
        def _():
            arrived(1)
            arrived(2)

        @pl.when(far_target)
        def _():
            arrived(0)

    fetch = pltpu.make_async_copy(ss_ref.at[0, rows, :], own, wsem.at[0])
    fetch.start()
    local_set(0)

    @pl.loop(1, sets)
    def _(a):
        local_set(a)

    barrier = pltpu.get_barrier_semaphore()

    def greet(to_tm, to_node):
        pl.semaphore_signal(barrier, inc=1, device_id=(to_tm, to_node), device_id_type=pl.DeviceIdType.MESH)

    def both(which_chip):
        for which in range(CORES):
            greet(dev(which_chip, which), node)

    greeted = jnp.int32(0)
    for cond, count, hello in (
        (has_next, 2, lambda: both(chip + 1)),
        (has_before, 2, lambda: both(chip - 1)),
        (far_source, 2, lambda: both(chip + 2)),
        (far_target, 1, lambda: greet(dev(chip - 2, 1), node)),
        (far_source, 1, lambda: greet(dev(middle, 0), node)),
        (far_middle, 1, lambda: greet(dev(source_chip, 1), node)),
        (far_middle, 2, lambda: both(target)),
        (far_target, 1, lambda: greet(dev(middle_of_target, 0), node)),
    ):
        pl.when(cond)(hello)
        greeted = greeted + jnp.where(cond, count, 0)
    greet(dev(chip, 1 - core), node)
    for by in range(1, M):
        for which in range(CORES):
            greet(dev(chip, which), lax.rem(node + by, M))
    for by in range(1, nz):
        greet(dev(ypos * nz + lax.rem(zpos + by, nz), core), node)
    for by in range(1, ny):
        greet(dev(lax.rem(ypos + by, ny) * nz + zpos, core), node)
    always = CORES * M - 1 + nz - 1 + ny - 1
    pl.semaphore_wait(barrier, greeted + always)
    fetch.wait()

    direct_set(0)
    near_set(0)

    @pl.loop(1, DIRECT + 1)
    def _(a):
        direct_set(a)
        near_set(a)

    @pl.loop(DIRECT + 1, sets)
    def _(a):
        first_leg(a)
        near_set(a)

    acc[...] = jnp.zeros_like(acc)
    first = chip == 0
    second = chip == 1
    width = TILE * LANES

    def force(ref, q, cw):
        x = ref[:, cols(q - 1, TILE + 2)]
        flux = cw * (pltpu.roll(x, (TILE + 2) * LANES - 1, axis=1) - x)
        spread = flux - pltpu.roll(flux, 1, axis=1)
        u = x[:, LANES:LANES + width]
        square = u * u
        g = u - u * square
        return u, square, g, spread[:, LANES:LANES + width] + g

    def newton(u, square, g, base, m):
        a = IMPLICIT[m]
        defect = base - u
        target = base - a * g
        once = u + defect / ((1.0 - a) + (3.0 * a) * square)
        square = once * once
        twice = (target + (2.0 * a) * square * once) / ((1.0 - a) + (3.0 * a) * square)
        return twice, defect

    def add_up(k, q, total):
        parts = []
        for t in range(TILE):
            mine = jnp.logical_and(q + t >= PAD, q + t < PAD + half)
            part = total[:, t * LANES:(t + 1) * LANES]
            parts.append(jnp.where(mine, part, jnp.zeros_like(part)))
        acc[k] += (parts[0] + parts[1]) + (parts[2] + parts[3])

    def start_sweep(q):
        cw = cbuf[:, cols(q - 1, TILE + 2)]
        here = cols(q, TILE)
        total = None
        for n in range(1, 5):
            u, square, g, f = force(buf.at[n], q, cw)
            before = buf[n - 1, :, here]
            if n == 3:
                before = jnp.where(first, u, before)
            if n == 1:
                before = jnp.where(second, u, before)
            for m in range(M):
                if n == 1 and m < M - 1:
                    continue
                new, defect = newton(u, square, g, before + ROW_SUMS[m] * f, m)
                if n == 1:
                    e1[:, here] = new
                else:
                    u1[n - 2, m, :, here] = new
                if n >= 3:
                    total = defect * defect if total is None else total + defect * defect
        add_up(0, q, total)

    def later_sweep(k, q):
        cw = cbuf[:, cols(q - 1, TILE + 2)]
        here = cols(q, TILE)
        total = None
        old = u1 if k == 1 else u2
        for n in range(2 if k == 1 else 3, 5):
            slot = n - 2 if k == 1 else n - 3
            parts = [force(old.at[slot, m], q, cw) for m in range(M)]
            if n == 2:
                before = e1[:, here]
            elif n == 3:
                before = u1[0, M - 1, :, here] if k == 1 else e2[:, here]
                before = jnp.where(first, buf[3, :, here], before)
            else:
                before = old[slot - 1, M - 1, :, here]
            for m in range(M):
                if n == 2 and m < M - 1:
                    continue
                base = before
                for j in range(M):
                    base = base + WEIGHTS[m][j] * parts[j][3]
                new, defect = newton(parts[m][0], parts[m][1], parts[m][2], base, m)
                if n == 2:
                    e2[:, here] = new
                elif k == 1:
                    u2[n - 3, m, :, here] = new
                else:
                    rbuf[n - 3, m, :, here] = new
                if n >= 3:
                    total = defect * defect if total is None else total + defect * defect
        add_up(k, q, total)

    def send_out(i):
        q = PAD + TILE * i
        place = cols(core * half + TILE * i, TILE)
        for away in range(M):
            to_node = lax.rem(node + away, M)
            for other in range(CORES):
                which = core if other == 0 else 1 - core
                src = rbuf.at[which, to_node, :, cols(q, TILE)]
                dst = out_ref.at[0, 0, rows, place]
                if away == 0 and other == 0:
                    pltpu.make_async_copy(src, dst, osend.at[0, 0]).start()
                else:
                    remote(src, dst, osend.at[other, away], orecv.at[other, away],
                           dev(chip, which), to_node).start()

    wait_set(0)

    @pl.loop(0, tiles + 1)
    def _(step):
        i = step - 1

        @pl.when(jnp.logical_and(far_middle, step + LEAD + 1 < sets))
        def _():
            second_leg(step + LEAD + 1)

        wait_set(step + 1)
        q = PAD + TILE * i
        start_sweep(q + 2)
        later_sweep(1, q + 1)
        later_sweep(2, q)

        @pl.when(step > 0)
        def _():
            send_out(i)

    lane = lax.broadcasted_iota(jnp.int32, (ROWS, LANES), 1)
    sums = jnp.zeros((ROWS, LANES), jnp.float32)
    for k in range(SWEEPS):
        sums = jnp.where(lane == k, jnp.sum(acc[k], axis=1, keepdims=True), sums)

    def swap(store, mine, value, peers, send, recv):
        store[mine] = value
        flows = [
            remote(store.at[mine], store.at[mine], send.at[by], recv.at[by], to_tm, to_node)
            for by, (to_tm, to_node) in enumerate(peers)
        ]
        for c in flows:
            c.start()
        for c in flows:
            c.wait()

    swap(st1, zpos, sums, [(dev(ypos * nz + lax.rem(zpos + by, nz), core), node) for by in range(1, nz)], s1s, s1r)
    sums = (st1[0] + st1[1]) + (st1[2] + st1[3])
    swap(st2, ypos, sums, [(dev(lax.rem(ypos + by, ny) * nz + zpos, core), node) for by in range(1, ny)], s2s, s2r)
    sums = (st2[0] + st2[1]) + (st2[2] + st2[3])
    me = node * CORES + core
    peers = [lax.rem(me + by, M * CORES) for by in range(1, M * CORES)]
    swap(st3, me, sums, [(dev(chip, lax.rem(p, CORES)), lax.div(p, CORES)) for p in peers], s3s, s3r)
    table = jnp.concatenate(
        [st3[CORES * m] + st3[CORES * m + 1] for m in range(M)]
        + [jnp.zeros((LANES - M * ROWS, LANES), jnp.float32)],
        axis=0,
    )
    table = jnp.log(log_floor + table.T / mean_count)
    res_ref[...] = table[:SWEEPS, :M * ROWS]

    def ended(flow, count):
        view = own.at[:, cols(0, count)]
        pltpu.make_async_copy(view, view, zsend.at[flow]).wait()

    ended(4, 1 + TILE * (sets - 1))

    @pl.when(has_next)
    def _():
        ended(0, 1 + TILE * (sets - 1))
        ended(1, 1 + TILE * (sets - 1))

    @pl.when(far_source)
    def _():
        for which in range(CORES):
            ended(2 + which, 1 + TILE * DIRECT)
            ended(5 + which, TILE * (sets - 1 - DIRECT))

    @pl.when(far_middle)
    def _():
        for which in range(CORES):
            ended(7 + which, TILE * (sets - 1 - DIRECT))

    made = rbuf.at[0, 0, :, cols(0, half)]
    for away in range(M):
        for other in range(CORES):
            pltpu.make_async_copy(made, made, osend.at[other, away]).wait()
            if away or other:
                pltpu.make_async_copy(made, made, orecv.at[other, away]).wait()


def body(sizes, slice_starts, coupling):
    systems, cells = coupling.shape
    ny, nz = sizes
    half = cells // LANES // CORES
    tiles = half // TILE
    span = half + PAD + TILE
    mean_count = float(ny * nz * CORES * M * cells)
    flat = lambda *lead: pltpu.VMEM(lead + (ROWS, span * LANES), jnp.float32)
    dma = pltpu.SemaphoreType.DMA
    any_spec = pl.BlockSpec(memory_space=pl.ANY)
    return pl.pallas_call(
        functools.partial(kernel, (ny, nz, cells, mean_count)),
        out_shape=(
            jax.ShapeDtypeStruct((1, 1, systems, cells), jnp.float32),
            jax.ShapeDtypeStruct((SWEEPS, systems), jnp.float32),
        ),
        in_specs=[pl.BlockSpec(memory_space=pltpu.HBM)] * 2,
        out_specs=(any_spec, pl.BlockSpec(memory_space=pltpu.VMEM)),
        scratch_shapes=[
            pltpu.VMEM((ROWS, cells), jnp.float32), flat(CORES),
            flat(5), flat(), flat(3, M), flat(), flat(2, M), flat(), flat(2, M),
            pltpu.VMEM((SWEEPS, ROWS, LANES), jnp.float32),
            pltpu.VMEM((nz, ROWS, LANES), jnp.float32),
            pltpu.VMEM((ny, ROWS, LANES), jnp.float32),
            pltpu.VMEM((M * CORES, ROWS, LANES), jnp.float32),
            dma((1,)), dma((tiles + 2,)), dma((5, tiles + 2)), dma((CORES, tiles + 2)), dma((9,)),
            dma((CORES, M)), dma((CORES, M)),
            dma((nz,)), dma((nz,)), dma((ny,)), dma((ny,)), dma((M * CORES,)), dma((M * CORES,)),
        ],
        compiler_params=pltpu.CompilerParams(
            collective_id=0, has_side_effects=True, vmem_limit_bytes=48 * 2**20
        ),
        name="sdc",
    )(slice_starts, coupling)


def solution(mesh):
    chips = mesh.shape["tm"] // CORES
    ny = 4
    return jax.shard_map(
        functools.partial(body, (ny, chips // ny)),
        mesh=mesh,
        in_specs=(P("tm", None, None), P()),
        out_specs=(P("tm", "node", None, None), P()),
        check_vma=False,
    )
```

```python
import functools

import jax
import jax.numpy as jnp
import numpy as np
from jax import lax
from jax.experimental import pallas as pl
from jax.experimental.pallas import tpu as pltpu
from jax.sharding import PartitionSpec as P

M = 4
SWEEPS = 3
CORES = 2
LANES = 128
ROWS = 8
TILE = 4
PAD = 5
time_step = 0.5
log_floor = 0.05


def legendre_gap(point, node_count):
    before = 1.0
    current = point
    for degree in range(1, node_count):
        following = ((2 * degree + 1) * point * current - degree * before) / (degree + 1)
        before = current
        current = following
    return current - before


def collocation(node_count):
    points = []
    samples = 4000
    for sample_index in range(samples - 1):
        lower_end = -1.0 + 2.0 * sample_index / samples
        upper_end = -1.0 + 2.0 * (sample_index + 1) / samples
        lower_value = legendre_gap(lower_end, node_count)
        upper_value = legendre_gap(upper_end, node_count)
        if lower_value * upper_value < 0.0:
            for halving in range(80):
                middle = 0.5 * (lower_end + upper_end)
                middle_value = legendre_gap(middle, node_count)
                if lower_value * middle_value <= 0.0:
                    upper_end = middle
                else:
                    lower_end = middle
                    lower_value = middle_value
            points.append(0.5 * (lower_end + upper_end))
    points.append(1.0)
    node_times = [(point + 1.0) / 2.0 for point in points]
    matrix = [[0.0] * node_count for row_index in range(node_count)]
    for column in range(node_count):
        coeffs = [1.0]
        for other in range(node_count):
            if other != column:
                scale = node_times[column] - node_times[other]
                shifted = [0.0] + coeffs
                scaled = [value * node_times[other] for value in coeffs] + [0.0]
                coeffs = [(shifted[power] - scaled[power]) / scale for power in range(len(shifted))]
        for row_index in range(node_count):
            upper_time = node_times[row_index]
            matrix[row_index][column] = sum(
                coeffs[power] * upper_time ** (power + 1) / (power + 1) for power in range(len(coeffs))
            )
    return (node_times, matrix)


NODE_TIMES, MATRIX = collocation(M)
WEIGHTS = [[time_step * float(np.float32(q)) for q in row] for row in MATRIX]
IMPLICIT = [float(np.float32(time_step * t / M)) for t in NODE_TIMES]
ROW_SUMS = [sum(row) for row in WEIGHTS]


LAG = 3
AHEAD = 3


def kernel(sizes, ss_ref, cp_ref, out_ref, res_ref, own, transit, buf, cbuf, u1, e1, u2, e2, rbuf, acc, st1, st2, st3,
           wsem, csem, rsem, tsem, zsend, osend, orecv, s1s, s1r, s2s, s2r, s3s, s3r):
    ny, nz, cells, mean_count = sizes
    half = cells // LANES // CORES
    tiles = half // TILE
    whole = cells // LANES
    chips = ny * nz
    sets = tiles + 2
    tm = lax.axis_index("tm")
    node = lax.axis_index("node")
    core = lax.rem(tm, CORES)
    chip = lax.div(tm, CORES)
    zpos = lax.rem(chip, nz)
    ypos = lax.div(chip, nz)
    rows = pl.ds(pl.multiple_of(node * ROWS, ROWS), ROWS)

    middle = jnp.where(zpos == 0, chip + nz - 1, chip - 1)
    source_chip = jnp.where(zpos == nz - 1, chip - nz + 1, chip + 1)
    target = jnp.where(zpos == nz - 1, chip - 1, chip + nz - 1)
    middle_of_target = jnp.where(zpos == 2, chip + 1, chip - nz + 1)
    has_next = chip < chips - 1
    has_before = chip > 0
    far_source = jnp.logical_and(core == 1, chip < chips - 2)
    far_target = chip > 1
    is_middle = source_chip < chips - 2
    far_middle = jnp.logical_and(core == 0, is_middle)

    def dev(which_chip, which):
        return which_chip * CORES + which

    def cols(start, count):
        if isinstance(start, int):
            return pl.ds(start * LANES, count * LANES)
        return pl.ds(pl.multiple_of(start * LANES, LANES), count * LANES)

    def remote(src, dst, send, recv, to_tm, to_node):
        return pltpu.make_async_remote_copy(
            src, dst, send, recv, device_id=(to_tm, to_node), device_id_type=pl.DeviceIdType.MESH
        )

    def source(which, a):
        if isinstance(a, int) and a == 0:
            return lax.rem(half * which + whole - 1, whole), PAD - 1, 1
        return lax.rem(half * which + TILE * (a - 1), whole), PAD + TILE * (a - 1), TILE

    def local_set(a):
        start, q, count = source(core, a)
        pltpu.make_async_copy(cp_ref.at[rows, cols(start, count)], cbuf.at[:, cols(q, count)], csem.at[a]).start()
        pltpu.make_async_copy(
            ss_ref.at[0, rows, cols(start, count)], buf.at[3 + core, :, cols(q, count)], rsem.at[3 + core, a]
        ).start()

    def near_set(a):
        @pl.when(has_next)
        def _():
            for which in range(CORES):
                start, q, count = source(which, a)
                remote(own.at[:, cols(start, count)], buf.at[1 + core, :, cols(q, count)],
                       zsend.at[which], rsem.at[1 + core, a], dev(chip + 1, which), node).start()

        start, q, count = source(1 - core, a)
        remote(own.at[:, cols(start, count)], buf.at[3 + core, :, cols(q, count)],
               zsend.at[4], rsem.at[3 + core, a], dev(chip, 1 - core), node).start()

    def first_leg(a):
        @pl.when(far_source)
        def _():
            for which in range(CORES):
                start, q, count = source(which, a)
                remote(own.at[:, cols(start, count)], transit.at[which, :, cols(q, count)],
                       zsend.at[2 + which], tsem.at[which, a], dev(middle, 0), node).start()

    def second_leg(a):
        for which in range(CORES):
            _, q, count = source(which, a)
            view = transit.at[which, :, cols(q, count)]
            pltpu.make_async_copy(view, view, tsem.at[which, a]).wait()
            remote(view, buf.at[0, :, cols(q, count)],
                   zsend.at[5 + which], rsem.at[0, a], dev(target, which), node).start()

    def wait_set(a):
        _, q, count = source(core, a)
        pltpu.make_async_copy(cbuf.at[:, cols(q, count)], cbuf.at[:, cols(q, count)], csem.at[a]).wait()

        def arrived(n):
            view = buf.at[n, :, cols(q, count)]
            pltpu.make_async_copy(view, view, rsem.at[n, a]).wait()

        arrived(3)
        arrived(4)

        @pl.when(has_before)
        def _():
            arrived(1)
            arrived(2)

    def wait_far_set(a):
        @pl.when(far_target)
        def _():
            _, q, count = source(core, a)
            view = buf.at[0, :, cols(q, count)]
            pltpu.make_async_copy(view, view, rsem.at[0, a]).wait()

    fetch = pltpu.make_async_copy(ss_ref.at[0, rows, :], own, wsem.at[0])
    fetch.start()
    local_set(0)

    @pl.loop(1, sets)
    def _(a):
        local_set(a)

    barrier = pltpu.get_barrier_semaphore()

    def greet(to_tm, to_node):
        pl.semaphore_signal(barrier, inc=1, device_id=(to_tm, to_node), device_id_type=pl.DeviceIdType.MESH)

    def both(which_chip):
        for which in range(CORES):
            greet(dev(which_chip, which), node)

    greeted = jnp.int32(0)
    for cond, count, hello in (
        (has_next, 2, lambda: both(chip + 1)),
        (has_before, 2, lambda: both(chip - 1)),
        (far_source, 1, lambda: greet(dev(middle, 0), node)),
        (far_middle, 1, lambda: greet(dev(source_chip, 1), node)),
        (far_middle, 2, lambda: both(target)),
        (far_target, 1, lambda: greet(dev(middle_of_target, 0), node)),
    ):
        pl.when(cond)(hello)
        greeted = greeted + jnp.where(cond, count, 0)
    greet(dev(chip, 1 - core), node)
    for by in range(1, M):
        for which in range(CORES):
            greet(dev(chip, which), lax.rem(node + by, M))
    for by in range(1, nz):
        greet(dev(ypos * nz + lax.rem(zpos + by, nz), core), node)
    for by in range(1, ny):
        greet(dev(lax.rem(ypos + by, ny) * nz + zpos, core), node)
    always = CORES * M - 1 + nz - 1 + ny - 1
    pl.semaphore_wait(barrier, greeted + always)
    fetch.wait()

    near_set(0)
    first_leg(0)

    @pl.loop(1, sets)
    def _(a):
        near_set(a)
        first_leg(a)

    acc[...] = jnp.zeros_like(acc)
    first = chip == 0
    second = chip == 1
    width = TILE * LANES

    def force(ref, q, cw):
        x = ref[:, cols(q - 1, TILE + 2)]
        flux = cw * (pltpu.roll(x, (TILE + 2) * LANES - 1, axis=1) - x)
        spread = flux - pltpu.roll(flux, 1, axis=1)
        u = x[:, LANES:LANES + width]
        square = u * u
        g = u - u * square
        return u, square, g, spread[:, LANES:LANES + width] + g

    def newton(u, square, g, base, m):
        a = IMPLICIT[m]
        defect = base - u
        target = base - a * g
        once = u + defect / ((1.0 - a) + (3.0 * a) * square)
        square = once * once
        twice = (target + (2.0 * a) * square * once) / ((1.0 - a) + (3.0 * a) * square)
        return twice, defect

    def add_up(k, q, total):
        whole_tile = None
        for t in range(TILE):
            mine = jnp.logical_and(q + t >= PAD, q + t < PAD + half)
            part = total[:, t * LANES:(t + 1) * LANES]
            part = jnp.where(mine, part, jnp.zeros_like(part))
            whole_tile = part if whole_tile is None else whole_tile + part
        acc[k] += whole_tile

    def start_sweep(q, slices):
        cw = cbuf[:, cols(q - 1, TILE + 2)]
        here = cols(q, TILE)
        total = None
        for n in slices:
            u, square, g, f = force(buf.at[n], q, cw)
            before = buf[n - 1, :, here]
            if n == 3:
                before = jnp.where(first, u, before)
            if n == 1:
                before = jnp.where(second, u, before)
            for m in range(M):
                if n == 1 and m < M - 1:
                    continue
                new, defect = newton(u, square, g, before + ROW_SUMS[m] * f, m)
                if n == 1:
                    e1[:, here] = new
                else:
                    u1[n - 2, m, :, here] = new
                if n >= 3:
                    total = defect * defect if total is None else total + defect * defect
        if total is not None:
            add_up(0, q, total)

    def later_sweep(k, q, slices):
        cw = cbuf[:, cols(q - 1, TILE + 2)]
        here = cols(q, TILE)
        total = None
        old = u1 if k == 1 else u2
        for n in slices:
            slot = n - 2 if k == 1 else n - 3
            parts = [force(old.at[slot, m], q, cw) for m in range(M)]
            if n == 2:
                before = e1[:, here]
            elif n == 3:
                before = u1[0, M - 1, :, here] if k == 1 else e2[:, here]
                before = jnp.where(first, buf[3, :, here], before)
            else:
                before = old[slot - 1, M - 1, :, here]
            for m in range(M):
                if n == 2 and m < M - 1:
                    continue
                base = before
                for j in range(M):
                    base = base + WEIGHTS[m][j] * parts[j][3]
                new, defect = newton(parts[m][0], parts[m][1], parts[m][2], base, m)
                if n == 2:
                    e2[:, here] = new
                elif k == 1:
                    u2[n - 3, m, :, here] = new
                else:
                    rbuf[n - 3, m, :, here] = new
                if n >= 3:
                    total = defect * defect if total is None else total + defect * defect
        if total is not None:
            add_up(k, q, total)

    def send_out(which, i):
        place = cols(core * half + TILE * i, TILE)
        for away in range(M):
            to_node = lax.rem(node + away, M)
            src = rbuf.at[which, to_node, :, cols(PAD + TILE * i, TILE)]
            dst = out_ref.at[0, 0, rows, place]
            out = remote(src, dst, osend.at[which, away], orecv.at[core, away], dev(chip, which), to_node)
            if away:
                out.start()
            else:
                pl.when(core != which)(out.start)
                pl.when(core == which)(pltpu.make_async_copy(src, dst, osend.at[which, 0]).start)

    wait_set(0)

    @pl.when(far_middle)
    def _():
        second_leg(0)

        @pl.loop(1, AHEAD)
        def _(a):
            second_leg(a)

    wait_far_set(0)

    @pl.loop(0, tiles + 1 + LAG)
    def _(step):
        @pl.when(jnp.logical_and(far_middle, step + AHEAD < sets))
        def _():
            second_leg(step + AHEAD)

        @pl.when(step <= tiles)
        def _():
            i = step - 1
            wait_set(step + 1)
            q = PAD + TILE * i
            start_sweep(q + 2, (4, 3, 2))
            later_sweep(1, q + 1, (4, 3))
            later_sweep(2, q, (4,))
            pl.when(i >= 0)(lambda: send_out(1, i))

        @pl.when(step >= LAG)
        def _():
            i = step - 1 - LAG
            wait_far_set(i + 2)
            q = PAD + TILE * i
            start_sweep(q + 2, (1,))
            later_sweep(1, q + 1, (2,))
            later_sweep(2, q, (3,))
            pl.when(i >= 0)(lambda: send_out(0, i))

    lane = lax.broadcasted_iota(jnp.int32, (ROWS, LANES), 1)
    sums = jnp.zeros((ROWS, LANES), jnp.float32)
    for k in range(SWEEPS):
        sums = jnp.where(lane == k, jnp.sum(acc[k], axis=1, keepdims=True), sums)

    def swap(store, mine, value, peers, send, recv):
        store[mine] = value
        flows = [
            remote(store.at[mine], store.at[mine], send.at[by], recv.at[by], to_tm, to_node)
            for by, (to_tm, to_node) in enumerate(peers)
        ]
        for c in flows:
            c.start()
        for c in flows:
            c.wait()

    swap(st1, zpos, sums, [(dev(ypos * nz + lax.rem(zpos + by, nz), core), node) for by in range(1, nz)], s1s, s1r)
    sums = (st1[0] + st1[1]) + (st1[2] + st1[3])
    swap(st2, ypos, sums, [(dev(lax.rem(ypos + by, ny) * nz + zpos, core), node) for by in range(1, ny)], s2s, s2r)
    sums = (st2[0] + st2[1]) + (st2[2] + st2[3])
    me = node * CORES + core
    peers = [lax.rem(me + by, M * CORES) for by in range(1, M * CORES)]
    swap(st3, me, sums, [(dev(chip, lax.rem(p, CORES)), lax.div(p, CORES)) for p in peers], s3s, s3r)
    table = jnp.concatenate(
        [st3[CORES * m] + st3[CORES * m + 1] for m in range(M)]
        + [jnp.zeros((LANES - M * ROWS, LANES), jnp.float32)],
        axis=0,
    )
    table = jnp.log(log_floor + table.T / mean_count)
    res_ref[...] = table[:SWEEPS, :M * ROWS]

    def ended(flow, count):
        view = own.at[:, cols(0, count)]
        pltpu.make_async_copy(view, view, zsend.at[flow]).wait()

    ended(4, 1 + TILE * (sets - 1))

    @pl.when(has_next)
    def _():
        ended(0, 1 + TILE * (sets - 1))
        ended(1, 1 + TILE * (sets - 1))

    @pl.when(far_source)
    def _():
        for which in range(CORES):
            ended(2 + which, 1 + TILE * (sets - 1))

    @pl.when(far_middle)
    def _():
        for which in range(CORES):
            ended(5 + which, 1 + TILE * (sets - 1))

    made = rbuf.at[0, 0, :, cols(0, half)]

    def drained(sem):
        pltpu.make_async_copy(made, made, sem).wait()

    for away in range(M):
        for which in range(CORES):
            drained(osend.at[which, away])
            if away:
                drained(orecv.at[which, away])
    drained(orecv.at[1 - core, 0])


def body(sizes, slice_starts, coupling):
    systems, cells = coupling.shape
    ny, nz = sizes
    half = cells // LANES // CORES
    tiles = half // TILE
    span = half + PAD + TILE
    mean_count = float(ny * nz * CORES * M * cells)
    flat = lambda *lead: pltpu.VMEM(lead + (ROWS, span * LANES), jnp.float32)
    dma = pltpu.SemaphoreType.DMA
    any_spec = pl.BlockSpec(memory_space=pl.ANY)
    return pl.pallas_call(
        functools.partial(kernel, (ny, nz, cells, mean_count)),
        out_shape=(
            jax.ShapeDtypeStruct((1, 1, systems, cells), jnp.float32),
            jax.ShapeDtypeStruct((SWEEPS, systems), jnp.float32),
        ),
        in_specs=[pl.BlockSpec(memory_space=pltpu.HBM)] * 2,
        out_specs=(any_spec, pl.BlockSpec(memory_space=pltpu.VMEM)),
        scratch_shapes=[
            pltpu.VMEM((ROWS, cells), jnp.float32), flat(CORES),
            flat(5), flat(), flat(3, M), flat(), flat(2, M), flat(), flat(2, M),
            pltpu.VMEM((SWEEPS, ROWS, LANES), jnp.float32),
            pltpu.VMEM((nz, ROWS, LANES), jnp.float32),
            pltpu.VMEM((ny, ROWS, LANES), jnp.float32),
            pltpu.VMEM((M * CORES, ROWS, LANES), jnp.float32),
            dma((1,)), dma((tiles + 2,)), dma((5, tiles + 2)), dma((CORES, tiles + 2)), dma((7,)),
            dma((CORES, M)), dma((CORES, M)),
            dma((nz,)), dma((nz,)), dma((ny,)), dma((ny,)), dma((M * CORES,)), dma((M * CORES,)),
        ],
        compiler_params=pltpu.CompilerParams(
            collective_id=0, has_side_effects=True, vmem_limit_bytes=48 * 2**20
        ),
        name="sdc",
    )(slice_starts, coupling)


def solution(mesh):
    chips = mesh.shape["tm"] // CORES
    ny = 4
    return jax.shard_map(
        functools.partial(body, (ny, chips // ny)),
        mesh=mesh,
        in_specs=(P("tm", None, None), P()),
        out_specs=(P("tm", "node", None, None), P()),
        check_vma=False,
    )
```

```python
import functools

import jax
import jax.numpy as jnp
import numpy as np
from jax import lax
from jax.experimental import pallas as pl
from jax.experimental.pallas import tpu as pltpu
from jax.sharding import PartitionSpec as P

M = 4
SWEEPS = 3
CORES = 2
LANES = 128
ROWS = 8
SUB = 2
TILE = 4
PAD = TILE + 1
time_step = 0.5
log_floor = 0.05


def legendre_gap(point, node_count):
    before = 1.0
    current = point
    for degree in range(1, node_count):
        following = ((2 * degree + 1) * point * current - degree * before) / (degree + 1)
        before = current
        current = following
    return current - before


def collocation(node_count):
    points = []
    samples = 4000
    for sample_index in range(samples - 1):
        lower_end = -1.0 + 2.0 * sample_index / samples
        upper_end = -1.0 + 2.0 * (sample_index + 1) / samples
        lower_value = legendre_gap(lower_end, node_count)
        upper_value = legendre_gap(upper_end, node_count)
        if lower_value * upper_value < 0.0:
            for halving in range(80):
                middle = 0.5 * (lower_end + upper_end)
                middle_value = legendre_gap(middle, node_count)
                if lower_value * middle_value <= 0.0:
                    upper_end = middle
                else:
                    lower_end = middle
                    lower_value = middle_value
            points.append(0.5 * (lower_end + upper_end))
    points.append(1.0)
    node_times = [(point + 1.0) / 2.0 for point in points]
    matrix = [[0.0] * node_count for row_index in range(node_count)]
    for column in range(node_count):
        coeffs = [1.0]
        for other in range(node_count):
            if other != column:
                scale = node_times[column] - node_times[other]
                shifted = [0.0] + coeffs
                scaled = [value * node_times[other] for value in coeffs] + [0.0]
                coeffs = [(shifted[power] - scaled[power]) / scale for power in range(len(shifted))]
        for row_index in range(node_count):
            upper_time = node_times[row_index]
            matrix[row_index][column] = sum(
                coeffs[power] * upper_time ** (power + 1) / (power + 1) for power in range(len(coeffs))
            )
    return (node_times, matrix)


NODE_TIMES, MATRIX = collocation(M)
WEIGHTS = [[time_step * float(np.float32(q)) for q in row] for row in MATRIX]
IMPLICIT = [float(np.float32(time_step * t / M)) for t in NODE_TIMES]
ROW_SUMS = [sum(row) for row in WEIGHTS]


LAG = 3
AHEAD = 3


SS = 0
CP, CL, CS = 5, 6, 7
U1 = 8
E1 = U1 + 3 * M * 3
U2 = E1 + 1
E2 = U2 + 2 * M * 3
OUT = E2 + 1
PLACES = OUT + 2 * M


def kernel(sizes, ss_ref, cp_ref, out_ref, res_ref, own, transit, arena, acc, st1, st2, st3,
           wsem, csem, rsem, tsem, zsend, osend, orecv, s1s, s1r, s2s, s2r, s3s, s3r):
    ny, nz, cells, mean_count = sizes
    half = cells // LANES // CORES
    tiles = half // TILE
    whole = cells // LANES
    chips = ny * nz
    sets = tiles + 2
    tm = lax.axis_index("tm")
    node = lax.axis_index("node")
    core = lax.rem(tm, CORES)
    chip = lax.div(tm, CORES)
    zpos = lax.rem(chip, nz)
    ypos = lax.div(chip, nz)
    rows = pl.ds(pl.multiple_of(node * ROWS, ROWS), ROWS)

    middle = jnp.where(zpos == 0, chip + nz - 1, chip - 1)
    source_chip = jnp.where(zpos == nz - 1, chip - nz + 1, chip + 1)
    target = jnp.where(zpos == nz - 1, chip - 1, chip + nz - 1)
    middle_of_target = jnp.where(zpos == 2, chip + 1, chip - nz + 1)
    has_next = chip < chips - 1
    has_before = chip > 0
    far_source = jnp.logical_and(core == 1, chip < chips - 2)
    far_target = chip > 1
    is_middle = source_chip < chips - 2
    far_middle = jnp.logical_and(core == 0, is_middle)

    def dev(which_chip, which):
        return which_chip * CORES + which

    def cols(start, count):
        if isinstance(start, int):
            return pl.ds(start * LANES, count * LANES)
        return pl.ds(pl.multiple_of(start * LANES, LANES), count * LANES)

    def remote(src, dst, send, recv, to_tm, to_node):
        return pltpu.make_async_remote_copy(
            src, dst, send, recv, device_id=(to_tm, to_node), device_id_type=pl.DeviceIdType.MESH
        )

    def source(which, a):
        if isinstance(a, int) and a == 0:
            return lax.rem(half * which + whole - 1, whole), PAD - 1, 1
        return lax.rem(half * which + TILE * (a - 1), whole), PAD + TILE * (a - 1), TILE

    def local_set(a):
        start, q, count = source(core, a)
        pltpu.make_async_copy(cp_ref.at[rows, cols(start, count)], arena.at[CP, :, cols(q, count)], csem.at[a]).start()
        pltpu.make_async_copy(
            ss_ref.at[0, rows, cols(start, count)], arena.at[3 + core, :, cols(q, count)], rsem.at[3 + core, a]
        ).start()

    def near_set(a):
        @pl.when(has_next)
        def _():
            for which in range(CORES):
                start, q, count = source(which, a)
                remote(own.at[:, cols(start, count)], arena.at[1 + core, :, cols(q, count)],
                       zsend.at[which], rsem.at[1 + core, a], dev(chip + 1, which), node).start()

        start, q, count = source(1 - core, a)
        remote(own.at[:, cols(start, count)], arena.at[3 + core, :, cols(q, count)],
               zsend.at[4], rsem.at[3 + core, a], dev(chip, 1 - core), node).start()

    def first_leg(a):
        @pl.when(far_source)
        def _():
            for which in range(CORES):
                start, q, count = source(which, a)
                remote(own.at[:, cols(start, count)], transit.at[which, :, cols(q, count)],
                       zsend.at[2 + which], tsem.at[which, a], dev(middle, 0), node).start()

    def second_leg(a):
        for which in range(CORES):
            _, q, count = source(which, a)
            view = transit.at[which, :, cols(q, count)]
            pltpu.make_async_copy(view, view, tsem.at[which, a]).wait()
            remote(view, arena.at[0, :, cols(q, count)],
                   zsend.at[5 + which], rsem.at[0, a], dev(target, which), node).start()

    def wait_set(a):
        _, q, count = source(core, a)
        pltpu.make_async_copy(arena.at[CP, :, cols(q, count)], arena.at[CP, :, cols(q, count)], csem.at[a]).wait()

        def arrived(n):
            view = arena.at[n, :, cols(q, count)]
            pltpu.make_async_copy(view, view, rsem.at[n, a]).wait()

        arrived(3)
        arrived(4)

        @pl.when(has_before)
        def _():
            arrived(1)
            arrived(2)

    def wait_far_set(a):
        @pl.when(far_target)
        def _():
            _, q, count = source(core, a)
            view = arena.at[0, :, cols(q, count)]
            pltpu.make_async_copy(view, view, rsem.at[0, a]).wait()

    fetch = pltpu.make_async_copy(ss_ref.at[0, rows, :], own, wsem.at[0])
    fetch.start()
    local_set(0)

    @pl.loop(1, sets)
    def _(a):
        local_set(a)

    barrier = pltpu.get_barrier_semaphore()

    def greet(to_tm, to_node):
        pl.semaphore_signal(barrier, inc=1, device_id=(to_tm, to_node), device_id_type=pl.DeviceIdType.MESH)

    def both(which_chip):
        for which in range(CORES):
            greet(dev(which_chip, which), node)

    greeted = jnp.int32(0)
    for cond, count, hello in (
        (has_next, 2, lambda: both(chip + 1)),
        (has_before, 2, lambda: both(chip - 1)),
        (far_source, 1, lambda: greet(dev(middle, 0), node)),
        (far_middle, 1, lambda: greet(dev(source_chip, 1), node)),
        (far_middle, 2, lambda: both(target)),
        (far_target, 1, lambda: greet(dev(middle_of_target, 0), node)),
    ):
        pl.when(cond)(hello)
        greeted = greeted + jnp.where(cond, count, 0)
    greet(dev(chip, 1 - core), node)
    for by in range(1, M):
        for which in range(CORES):
            greet(dev(chip, which), lax.rem(node + by, M))
    for by in range(1, nz):
        greet(dev(ypos * nz + lax.rem(zpos + by, nz), core), node)
    for by in range(1, ny):
        greet(dev(lax.rem(ypos + by, ny) * nz + zpos, core), node)
    always = CORES * M - 1 + nz - 1 + ny - 1
    pl.semaphore_wait(barrier, greeted + always)
    fetch.wait()

    near_set(0)
    first_leg(0)

    @pl.loop(1, sets)
    def _(a):
        near_set(a)
        first_leg(a)

    acc[...] = jnp.zeros_like(acc)
    first = chip == 0
    second = chip == 1
    width = SUB * LANES
    lane = lax.broadcasted_iota(jnp.int32, (ROWS, width), 1) % LANES
    low = lane == 0
    high = lane == LANES - 1

    def load(v, place, q, count=SUB):
        return v[place, :, cols(q, count)]

    def piece(value, t):
        return value[:, t * LANES:(t + 1) * LANES]

    def rolled(v, place, q, count, by):
        return jnp.concatenate([pltpu.roll(load(v, place, q + t, 1), by, axis=1) for t in range(count)], axis=1)

    def pick_right(turned):
        return jnp.where(high, turned[:, LANES:], turned[:, :width])

    def pick_left(turned):
        return jnp.where(low, turned[:, :width], turned[:, LANES:])

    def force(u, square, right, left, parts):
        c, cl, cs = parts
        return c * right + cl * left + u * (cs - square)

    def newton(u, square3, defect, target, m):
        a = IMPLICIT[m]
        once = u + defect / ((1.0 - a) + square3)
        square = once * once
        return (target + (2.0 * a) * square * once) / ((1.0 - a) + (3.0 * a) * square)

    def keep(v, place, q, new):
        for t in range(SUB):
            part = piece(new, t)
            v[place, :, cols(q + t, 1)] = part
            v[place + 1, :, cols(q + t, 1)] = pltpu.roll(part, LANES - 1, axis=1)
            v[place + 2, :, cols(q + t, 1)] = pltpu.roll(part, 1, axis=1)

    def add_up(k, q, total):
        whole_tile = None
        for t in range(SUB):
            mine = jnp.logical_and(q + t >= PAD, q + t < PAD + half)
            part = jnp.where(mine, piece(total, t), jnp.zeros((ROWS, LANES), jnp.float32))
            whole_tile = part if whole_tile is None else whole_tile + part
        acc[k] += whole_tile

    def start_sweep(v, first_col, q, slices):
        here = cols(q, SUB)
        c = load(v, CP, q)
        if 1 in slices:
            parts = (c, load(v, CL, q), load(v, CS, q))
        else:
            cl = pick_left(rolled(v, CP, q - 1, SUB + 1, 1))
            cs = 1.0 - (c + cl)
            v[CL, :, here] = cl
            v[CS, :, here] = cs
            parts = (c, cl, cs)
        total = None
        for n in slices:
            u = load(v, SS + n, q)
            square = u * u
            f = force(u, square, pick_right(rolled(v, SS + n, q, SUB + 1, LANES - 1)),
                      pick_left(rolled(v, SS + n, q - 1, SUB + 1, 1)), parts)
            before = load(v, SS + n - 1, q)
            if n == 3:
                before = jnp.where(first, u, before)
            if n == 1:
                before = jnp.where(second, u, before)
            pull = f - 0.25 * (u - u * square)
            gap = before - u
            for m in range(M):
                if n == 1 and m < M - 1:
                    continue
                defect = gap + ROW_SUMS[m] * f
                new = newton(u, (3.0 * IMPLICIT[m]) * square, defect, before + ROW_SUMS[m] * pull, m)
                if n == 1:
                    v[E1, :, here] = new
                else:
                    keep(v, U1 + ((n - 2) * M + m) * 3, q, new)
                if n >= 3:
                    total = defect * defect if total is None else total + defect * defect
        if total is not None:
            add_up(0, first_col + q, total)

    def later_sweep(v, first_col, k, q, slices):
        here = cols(q, SUB)
        parts = (load(v, CP, q), load(v, CL, q), load(v, CS, q))
        total = None
        for n in slices:
            at = U1 + (n - 2) * M * 3 if k == 1 else U2 + (n - 3) * M * 3
            us, squares, forces = [], [], []
            for m in range(M):
                u = load(v, at + 3 * m, q)
                square = u * u
                right = pick_right(load(v, at + 3 * m + 1, q, SUB + 1))
                left = pick_left(load(v, at + 3 * m + 2, q - 1, SUB + 1))
                us.append(u)
                squares.append(square)
                forces.append(force(u, square, right, left, parts))
            if n == 2:
                before = load(v, E1, q)
            elif n == 3:
                before = load(v, U1 + (M - 1) * 3 if k == 1 else E2, q)
                before = jnp.where(first, load(v, SS + 3, q), before)
            else:
                before = load(v, at - 3, q)
            for m in range(M):
                if n == 2 and m < M - 1:
                    continue
                base = before
                for j in range(M):
                    base = base + WEIGHTS[m][j] * forces[j]
                a = IMPLICIT[m]
                defect = base - us[m]
                scaled = a * squares[m]
                target = defect + us[m] * ((1.0 - a) + scaled)
                new = newton(us[m], 3.0 * scaled, defect, target, m)
                if n == 2:
                    v[E2, :, here] = new
                elif k == 1:
                    keep(v, U2 + ((n - 3) * M + m) * 3, q, new)
                else:
                    v[OUT + (n - 3) * M + m, :, here] = new
                if n >= 3:
                    total = defect * defect if total is None else total + defect * defect
        if total is not None:
            add_up(k, first_col + q, total)

    def window(step):
        return arena.at[:, :, cols(step * TILE, TILE + 6)], step * TILE

    def main_part(step):
        v, at = window(step)
        for g in range(0, TILE, SUB):
            start_sweep(v, at, 3 + g, (4, 3, 2))
        for g in range(0, TILE, SUB):
            later_sweep(v, at, 1, 2 + g, (4, 3))
        for g in range(0, TILE, SUB):
            later_sweep(v, at, 2, 1 + g, (4,))

    def lagging_part(step):
        v, at = window(step)
        for g in range(0, TILE, SUB):
            start_sweep(v, at, 3 + g, (1,))
        for g in range(0, TILE, SUB):
            later_sweep(v, at, 1, 2 + g, (2,))
        for g in range(0, TILE, SUB):
            later_sweep(v, at, 2, 1 + g, (3,))

    def send_out(which, i):
        place = cols(core * half + TILE * i, TILE)
        for away in range(M):
            to_node = lax.rem(node + away, M)
            src = arena.at[OUT + which * M + to_node, :, cols(PAD + TILE * i, TILE)]
            dst = out_ref.at[0, 0, rows, place]
            out = remote(src, dst, osend.at[which, away], orecv.at[core, away], dev(chip, which), to_node)
            if away:
                out.start()
            else:
                pl.when(core != which)(out.start)
                pl.when(core == which)(pltpu.make_async_copy(src, dst, osend.at[which, 0]).start)

    wait_set(0)

    @pl.when(far_middle)
    def _():
        second_leg(0)

        @pl.loop(1, AHEAD)
        def _(a):
            second_leg(a)

    wait_far_set(0)

    @pl.loop(0, tiles + 1 + LAG)
    def _(step):
        @pl.when(jnp.logical_and(far_middle, step + AHEAD < sets))
        def _():
            second_leg(step + AHEAD)

        @pl.when(step <= tiles)
        def _():
            i = step - 1
            wait_set(step + 1)
            main_part(step)
            pl.when(i >= 0)(lambda: send_out(1, i))

        @pl.when(step >= LAG)
        def _():
            i = step - 1 - LAG
            wait_far_set(i + 2)
            lagging_part(step - LAG)
            pl.when(i >= 0)(lambda: send_out(0, i))

    column = lax.broadcasted_iota(jnp.int32, (ROWS, LANES), 1)
    sums = jnp.zeros((ROWS, LANES), jnp.float32)
    for k in range(SWEEPS):
        sums = jnp.where(column == k, jnp.sum(acc[k], axis=1, keepdims=True), sums)

    def swap(store, mine, value, peers, send, recv):
        store[mine] = value
        flows = [
            remote(store.at[mine], store.at[mine], send.at[by], recv.at[by], to_tm, to_node)
            for by, (to_tm, to_node) in enumerate(peers)
        ]
        for c in flows:
            c.start()
        for c in flows:
            c.wait()

    swap(st1, zpos, sums, [(dev(ypos * nz + lax.rem(zpos + by, nz), core), node) for by in range(1, nz)], s1s, s1r)
    sums = (st1[0] + st1[1]) + (st1[2] + st1[3])
    swap(st2, ypos, sums, [(dev(lax.rem(ypos + by, ny) * nz + zpos, core), node) for by in range(1, ny)], s2s, s2r)
    sums = (st2[0] + st2[1]) + (st2[2] + st2[3])
    me = node * CORES + core
    peers = [lax.rem(me + by, M * CORES) for by in range(1, M * CORES)]
    swap(st3, me, sums, [(dev(chip, lax.rem(p, CORES)), lax.div(p, CORES)) for p in peers], s3s, s3r)
    table = jnp.concatenate(
        [st3[CORES * m] + st3[CORES * m + 1] for m in range(M)]
        + [jnp.zeros((LANES - M * ROWS, LANES), jnp.float32)],
        axis=0,
    )
    table = jnp.log(log_floor + table.T / mean_count)
    res_ref[...] = table[:SWEEPS, :M * ROWS]

    def ended(flow, count):
        view = own.at[:, cols(0, count)]
        pltpu.make_async_copy(view, view, zsend.at[flow]).wait()

    ended(4, 1 + TILE * (sets - 1))

    @pl.when(has_next)
    def _():
        ended(0, 1 + TILE * (sets - 1))
        ended(1, 1 + TILE * (sets - 1))

    @pl.when(far_source)
    def _():
        for which in range(CORES):
            ended(2 + which, 1 + TILE * (sets - 1))

    @pl.when(far_middle)
    def _():
        for which in range(CORES):
            ended(5 + which, 1 + TILE * (sets - 1))

    made = arena.at[OUT, :, cols(0, half)]

    def drained(sem):
        pltpu.make_async_copy(made, made, sem).wait()

    for away in range(M):
        for which in range(CORES):
            drained(osend.at[which, away])
            if away:
                drained(orecv.at[which, away])
    drained(orecv.at[1 - core, 0])


def body(sizes, slice_starts, coupling):
    systems, cells = coupling.shape
    ny, nz = sizes
    half = cells // LANES // CORES
    tiles = half // TILE
    span = half + 2 * TILE + 6
    mean_count = float(ny * nz * CORES * M * cells)
    flat = lambda *lead: pltpu.VMEM(lead + (ROWS, span * LANES), jnp.float32)
    dma = pltpu.SemaphoreType.DMA
    any_spec = pl.BlockSpec(memory_space=pl.ANY)
    return pl.pallas_call(
        functools.partial(kernel, (ny, nz, cells, mean_count)),
        out_shape=(
            jax.ShapeDtypeStruct((1, 1, systems, cells), jnp.float32),
            jax.ShapeDtypeStruct((SWEEPS, systems), jnp.float32),
        ),
        in_specs=[pl.BlockSpec(memory_space=pltpu.HBM)] * 2,
        out_specs=(any_spec, pl.BlockSpec(memory_space=pltpu.VMEM)),
        scratch_shapes=[
            pltpu.VMEM((ROWS, cells), jnp.float32), flat(CORES), flat(PLACES),
            pltpu.VMEM((SWEEPS, ROWS, LANES), jnp.float32),
            pltpu.VMEM((nz, ROWS, LANES), jnp.float32),
            pltpu.VMEM((ny, ROWS, LANES), jnp.float32),
            pltpu.VMEM((M * CORES, ROWS, LANES), jnp.float32),
            dma((1,)), dma((tiles + 2,)), dma((5, tiles + 2)), dma((CORES, tiles + 2)), dma((7,)),
            dma((CORES, M)), dma((CORES, M)),
            dma((nz,)), dma((nz,)), dma((ny,)), dma((ny,)), dma((M * CORES,)), dma((M * CORES,)),
        ],
        compiler_params=pltpu.CompilerParams(
            collective_id=0, has_side_effects=True, vmem_limit_bytes=48 * 2**20
        ),
        name="sdc",
    )(slice_starts, coupling)


def solution(mesh):
    chips = mesh.shape["tm"] // CORES
    ny = 4
    return jax.shard_map(
        functools.partial(body, (ny, chips // ny)),
        mesh=mesh,
        in_specs=(P("tm", None, None), P()),
        out_specs=(P("tm", "node", None, None), P()),
        check_vma=False,
    )
```

```python
import functools

import jax
import jax.numpy as jnp
import numpy as np
from jax import lax
from jax.experimental import pallas as pl
from jax.experimental.pallas import tpu as pltpu
from jax.sharding import PartitionSpec as P

M = 4
SWEEPS = 3
CORES = 2
LANES = 128
ROWS = 8
SUB = 2
TILE = 4
PAD = TILE + 1
time_step = 0.5
log_floor = 0.05


def legendre_gap(point, node_count):
    before = 1.0
    current = point
    for degree in range(1, node_count):
        following = ((2 * degree + 1) * point * current - degree * before) / (degree + 1)
        before = current
        current = following
    return current - before


def collocation(node_count):
    points = []
    samples = 4000
    for sample_index in range(samples - 1):
        lower_end = -1.0 + 2.0 * sample_index / samples
        upper_end = -1.0 + 2.0 * (sample_index + 1) / samples
        lower_value = legendre_gap(lower_end, node_count)
        upper_value = legendre_gap(upper_end, node_count)
        if lower_value * upper_value < 0.0:
            for halving in range(80):
                middle = 0.5 * (lower_end + upper_end)
                middle_value = legendre_gap(middle, node_count)
                if lower_value * middle_value <= 0.0:
                    upper_end = middle
                else:
                    lower_end = middle
                    lower_value = middle_value
            points.append(0.5 * (lower_end + upper_end))
    points.append(1.0)
    node_times = [(point + 1.0) / 2.0 for point in points]
    matrix = [[0.0] * node_count for row_index in range(node_count)]
    for column in range(node_count):
        coeffs = [1.0]
        for other in range(node_count):
            if other != column:
                scale = node_times[column] - node_times[other]
                shifted = [0.0] + coeffs
                scaled = [value * node_times[other] for value in coeffs] + [0.0]
                coeffs = [(shifted[power] - scaled[power]) / scale for power in range(len(shifted))]
        for row_index in range(node_count):
            upper_time = node_times[row_index]
            matrix[row_index][column] = sum(
                coeffs[power] * upper_time ** (power + 1) / (power + 1) for power in range(len(coeffs))
            )
    return (node_times, matrix)


NODE_TIMES, MATRIX = collocation(M)
WEIGHTS = [[time_step * float(np.float32(q)) for q in row] for row in MATRIX]
IMPLICIT = [float(np.float32(time_step * t / M)) for t in NODE_TIMES]
ROW_SUMS = [sum(row) for row in WEIGHTS]


LAG = 3
AHEAD = 3


SS = 0
CP, CL, CS = 5, 6, 7
U1 = 8
E1 = U1 + 3 * M * 3
U2 = E1 + 1
E2 = U2 + 2 * M * 3
OUT = E2 + 1
PLACES = OUT + 2 * M


def kernel(sizes, ss_ref, cp_ref, out_ref, sums_ref, own, transit, arena, acc, st1, st2, st3,
           wsem, csem, rsem, tsem, zsend, osend, orecv, s1s, s1r, s2s, s2r, s3s, s3r):
    ny, nz, cells = sizes
    half = cells // LANES // CORES
    tiles = half // TILE
    whole = cells // LANES
    chips = ny * nz
    sets = tiles + 2
    tm = lax.axis_index("tm")
    node = lax.axis_index("node")
    core = lax.rem(tm, CORES)
    chip = lax.div(tm, CORES)
    zpos = lax.rem(chip, nz)
    ypos = lax.div(chip, nz)
    rows = pl.ds(pl.multiple_of(node * ROWS, ROWS), ROWS)

    middle = jnp.where(zpos == 0, chip + nz - 1, chip - 1)
    source_chip = jnp.where(zpos == nz - 1, chip - nz + 1, chip + 1)
    target = jnp.where(zpos == nz - 1, chip - 1, chip + nz - 1)
    middle_of_target = jnp.where(zpos == 2, chip + 1, chip - nz + 1)
    has_next = chip < chips - 1
    has_before = chip > 0
    far_source = jnp.logical_and(core == 1, chip < chips - 2)
    far_target = chip > 1
    is_middle = source_chip < chips - 2
    far_middle = jnp.logical_and(core == 0, is_middle)

    def dev(which_chip, which):
        return which_chip * CORES + which

    def cols(start, count):
        if isinstance(start, int):
            return pl.ds(start * LANES, count * LANES)
        return pl.ds(pl.multiple_of(start * LANES, LANES), count * LANES)

    def remote(src, dst, send, recv, to_tm, to_node):
        return pltpu.make_async_remote_copy(
            src, dst, send, recv, device_id=(to_tm, to_node), device_id_type=pl.DeviceIdType.MESH
        )

    def source(which, a):
        if isinstance(a, int) and a == 0:
            return lax.rem(half * which + whole - 1, whole), PAD - 1, 1
        count = 1 if isinstance(a, int) and a == sets - 1 else TILE
        return lax.rem(half * which + TILE * (a - 1), whole), PAD + TILE * (a - 1), count

    def each_set(a, what):
        pl.when(a < sets - 1)(lambda: what(a))
        pl.when(a == sets - 1)(lambda: what(sets - 1))

    def local_set(a):
        start, q, count = source(core, a)
        pltpu.make_async_copy(cp_ref.at[rows, cols(start, count)], arena.at[CP, :, cols(q, count)], csem.at[a]).start()
        pltpu.make_async_copy(
            ss_ref.at[0, rows, cols(start, count)], arena.at[3 + core, :, cols(q, count)], rsem.at[3 + core, a]
        ).start()

    def near_set(a):
        @pl.when(has_next)
        def _():
            for which in range(CORES):
                start, q, count = source(which, a)
                remote(own.at[:, cols(start, count)], arena.at[1 + core, :, cols(q, count)],
                       zsend.at[which], rsem.at[1 + core, a], dev(chip + 1, which), node).start()

        start, q, count = source(1 - core, a)
        remote(own.at[:, cols(start, count)], arena.at[3 + core, :, cols(q, count)],
               zsend.at[4], rsem.at[3 + core, a], dev(chip, 1 - core), node).start()

    def first_leg(a):
        @pl.when(far_source)
        def _():
            for which in range(CORES):
                start, q, count = source(which, a)
                remote(own.at[:, cols(start, count)], transit.at[which, :, cols(q, count)],
                       zsend.at[2 + which], tsem.at[which, a], dev(middle, 0), node).start()

    def second_leg(a):
        for which in range(CORES):
            _, q, count = source(which, a)
            view = transit.at[which, :, cols(q, count)]
            pltpu.make_async_copy(view, view, tsem.at[which, a]).wait()
            remote(view, arena.at[0, :, cols(q, count)],
                   zsend.at[5 + which], rsem.at[0, a], dev(target, which), node).start()

    def wait_set(a):
        _, q, count = source(core, a)
        pltpu.make_async_copy(arena.at[CP, :, cols(q, count)], arena.at[CP, :, cols(q, count)], csem.at[a]).wait()

        def arrived(n):
            view = arena.at[n, :, cols(q, count)]
            pltpu.make_async_copy(view, view, rsem.at[n, a]).wait()

        arrived(3)
        arrived(4)

        @pl.when(has_before)
        def _():
            arrived(1)
            arrived(2)

    def wait_far_set(a):
        @pl.when(far_target)
        def _():
            _, q, count = source(core, a)
            view = arena.at[0, :, cols(q, count)]
            pltpu.make_async_copy(view, view, rsem.at[0, a]).wait()

    fetch = pltpu.make_async_copy(ss_ref.at[0, rows, :], own, wsem.at[0])
    fetch.start()
    local_set(0)

    @pl.loop(1, sets - 1)
    def _(a):
        local_set(a)

    local_set(sets - 1)

    barrier = pltpu.get_barrier_semaphore()

    def greet(to_tm, to_node):
        pl.semaphore_signal(barrier, inc=1, device_id=(to_tm, to_node), device_id_type=pl.DeviceIdType.MESH)

    def both(which_chip):
        for which in range(CORES):
            greet(dev(which_chip, which), node)

    greeted = jnp.int32(0)
    for cond, count, hello in (
        (has_next, 2, lambda: both(chip + 1)),
        (has_before, 2, lambda: both(chip - 1)),
        (far_source, 1, lambda: greet(dev(middle, 0), node)),
        (far_middle, 1, lambda: greet(dev(source_chip, 1), node)),
        (far_middle, 2, lambda: both(target)),
        (far_target, 1, lambda: greet(dev(middle_of_target, 0), node)),
    ):
        pl.when(cond)(hello)
        greeted = greeted + jnp.where(cond, count, 0)
    greet(dev(chip, 1 - core), node)
    for by in range(1, M):
        for which in range(CORES):
            greet(dev(chip, which), lax.rem(node + by, M))
    for by in range(1, nz):
        greet(dev(ypos * nz + lax.rem(zpos + by, nz), core), node)
    for by in range(1, ny):
        greet(dev(lax.rem(ypos + by, ny) * nz + zpos, core), node)
    always = CORES * M - 1 + nz - 1 + ny - 1
    pl.semaphore_wait(barrier, greeted + always)
    fetch.wait()

    near_set(0)
    first_leg(0)

    @pl.loop(1, sets - 1)
    def _(a):
        near_set(a)
        first_leg(a)

    near_set(sets - 1)
    first_leg(sets - 1)

    acc[...] = jnp.zeros_like(acc)
    first = chip == 0
    second = chip == 1
    width = SUB * LANES
    lane = lax.broadcasted_iota(jnp.int32, (ROWS, width), 1) % LANES
    low = lane == 0
    high = lane == LANES - 1

    def load(v, place, q, count=SUB):
        return v[place, :, cols(q, count)]

    def piece(value, t):
        return value[:, t * LANES:(t + 1) * LANES]

    def rolled(v, place, q, count, by):
        return jnp.concatenate([pltpu.roll(load(v, place, q + t, 1), by, axis=1) for t in range(count)], axis=1)

    def pick_right(turned):
        return jnp.where(high, turned[:, LANES:], turned[:, :width])

    def pick_left(turned):
        return jnp.where(low, turned[:, :width], turned[:, LANES:])

    def force(u, square, right, left, parts):
        c, cl, cs = parts
        return c * right + cl * left + u * (cs - square)

    def newton(u, square3, defect, target, m):
        a = IMPLICIT[m]
        once = u + defect / ((1.0 - a) + square3)
        square = once * once
        return (target + (2.0 * a) * square * once) / ((1.0 - a) + (3.0 * a) * square)

    def keep(v, place, q, new):
        for t in range(SUB):
            part = piece(new, t)
            v[place, :, cols(q + t, 1)] = part
            v[place + 1, :, cols(q + t, 1)] = pltpu.roll(part, LANES - 1, axis=1)
            v[place + 2, :, cols(q + t, 1)] = pltpu.roll(part, 1, axis=1)

    def add_up(k, q, total):
        whole_tile = None
        for t in range(SUB):
            mine = jnp.logical_and(q + t >= PAD, q + t < PAD + half)
            part = jnp.where(mine, piece(total, t), jnp.zeros((ROWS, LANES), jnp.float32))
            whole_tile = part if whole_tile is None else whole_tile + part
        acc[k] += whole_tile

    def start_sweep(v, first_col, q, slices):
        here = cols(q, SUB)
        c = load(v, CP, q)
        if 1 in slices:
            parts = (c, load(v, CL, q), load(v, CS, q))
        else:
            cl = pick_left(rolled(v, CP, q - 1, SUB + 1, 1))
            cs = 1.0 - (c + cl)
            v[CL, :, here] = cl
            v[CS, :, here] = cs
            parts = (c, cl, cs)
        total = None
        for n in slices:
            u = load(v, SS + n, q)
            square = u * u
            f = force(u, square, pick_right(rolled(v, SS + n, q, SUB + 1, LANES - 1)),
                      pick_left(rolled(v, SS + n, q - 1, SUB + 1, 1)), parts)
            before = load(v, SS + n - 1, q)
            if n == 3:
                before = jnp.where(first, u, before)
            if n == 1:
                before = jnp.where(second, u, before)
            pull = f - 0.25 * (u - u * square)
            gap = before - u
            for m in range(M):
                if n == 1 and m < M - 1:
                    continue
                defect = gap + ROW_SUMS[m] * f
                new = newton(u, (3.0 * IMPLICIT[m]) * square, defect, before + ROW_SUMS[m] * pull, m)
                if n == 1:
                    v[E1, :, here] = new
                else:
                    keep(v, U1 + ((n - 2) * M + m) * 3, q, new)
                if n >= 3:
                    total = defect * defect if total is None else total + defect * defect
        if total is not None:
            add_up(0, first_col + q, total)

    def later_sweep(v, first_col, k, q, slices):
        here = cols(q, SUB)
        parts = (load(v, CP, q), load(v, CL, q), load(v, CS, q))
        total = None
        for n in slices:
            at = U1 + (n - 2) * M * 3 if k == 1 else U2 + (n - 3) * M * 3
            us, squares, forces = [], [], []
            for m in range(M):
                u = load(v, at + 3 * m, q)
                square = u * u
                right = pick_right(load(v, at + 3 * m + 1, q, SUB + 1))
                left = pick_left(load(v, at + 3 * m + 2, q - 1, SUB + 1))
                us.append(u)
                squares.append(square)
                forces.append(force(u, square, right, left, parts))
            if n == 2:
                before = load(v, E1, q)
            elif n == 3:
                before = load(v, U1 + (M - 1) * 3 if k == 1 else E2, q)
                before = jnp.where(first, load(v, SS + 3, q), before)
            else:
                before = load(v, at - 3, q)
            for m in range(M):
                if n == 2 and m < M - 1:
                    continue
                base = before
                for j in range(M):
                    base = base + WEIGHTS[m][j] * forces[j]
                a = IMPLICIT[m]
                defect = base - us[m]
                scaled = a * squares[m]
                target = defect + us[m] * ((1.0 - a) + scaled)
                new = newton(us[m], 3.0 * scaled, defect, target, m)
                if n == 2:
                    v[E2, :, here] = new
                elif k == 1:
                    keep(v, U2 + ((n - 3) * M + m) * 3, q, new)
                else:
                    v[OUT + (n - 3) * M + m, :, here] = new
                if n >= 3:
                    total = defect * defect if total is None else total + defect * defect
        if total is not None:
            add_up(k, first_col + q, total)

    def window(step):
        return arena.at[:, :, cols(step * TILE, TILE + 6)], step * TILE

    def main_part(step):
        v, at = window(step)
        for g in range(0, TILE, SUB):
            start_sweep(v, at, 3 + g, (4, 3, 2))
        for g in range(0, TILE, SUB):
            later_sweep(v, at, 1, 2 + g, (4, 3))
        for g in range(0, TILE, SUB):
            later_sweep(v, at, 2, 1 + g, (4,))

    def lagging_part(step):
        v, at = window(step)
        for g in range(0, TILE, SUB):
            start_sweep(v, at, 3 + g, (1,))
        for g in range(0, TILE, SUB):
            later_sweep(v, at, 1, 2 + g, (2,))
        for g in range(0, TILE, SUB):
            later_sweep(v, at, 2, 1 + g, (3,))

    def send_out(which, i):
        place = cols(core * half + TILE * i, TILE)
        for away in range(M):
            to_node = lax.rem(node + away, M)
            src = arena.at[OUT + which * M + to_node, :, cols(PAD + TILE * i, TILE)]
            dst = out_ref.at[0, 0, rows, place]
            out = remote(src, dst, osend.at[which, away], orecv.at[core, away], dev(chip, which), to_node)
            if away:
                out.start()
            else:
                pl.when(core != which)(out.start)
                pl.when(core == which)(pltpu.make_async_copy(src, dst, osend.at[which, 0]).start)

    wait_set(0)

    @pl.when(far_middle)
    def _():
        second_leg(0)

        @pl.loop(1, AHEAD)
        def _(a):
            second_leg(a)

    wait_far_set(0)

    @pl.loop(0, tiles + 1 + LAG)
    def _(step):
        @pl.when(far_middle)
        def _():
            each_set(step + AHEAD, second_leg)

        @pl.when(step <= tiles)
        def _():
            i = step - 1
            each_set(step + 1, wait_set)
            main_part(step)
            pl.when(i >= 0)(lambda: send_out(1, i))

        @pl.when(step >= LAG)
        def _():
            i = step - 1 - LAG
            each_set(i + 2, wait_far_set)
            lagging_part(step - LAG)
            pl.when(i >= 0)(lambda: send_out(0, i))

    row = lax.broadcasted_iota(jnp.int32, (ROWS, LANES), 0)
    column = lax.broadcasted_iota(jnp.int32, (ROWS, LANES), 1)
    place = column == node * ROWS + row
    sums = jnp.zeros((ROWS, LANES), jnp.float32)
    for k in range(SWEEPS):
        spread = jnp.where(place, jnp.sum(acc[k], axis=1, keepdims=True), 0.0)
        sums = jnp.where(row == k, jnp.sum(spread, axis=0, keepdims=True), sums)

    def swap(store, mine, value, peers, send, recv):
        store[mine] = value
        flows = [
            remote(store.at[mine], store.at[mine], send.at[by], recv.at[by], to_tm, to_node)
            for by, (to_tm, to_node) in enumerate(peers)
        ]
        for c in flows:
            c.start()
        for c in flows:
            c.wait()

    swap(st1, zpos, sums, [(dev(ypos * nz + lax.rem(zpos + by, nz), core), node) for by in range(1, nz)], s1s, s1r)
    sums = (st1[0] + st1[1]) + (st1[2] + st1[3])
    swap(st2, ypos, sums, [(dev(lax.rem(ypos + by, ny) * nz + zpos, core), node) for by in range(1, ny)], s2s, s2r)
    sums = (st2[0] + st2[1]) + (st2[2] + st2[3])
    me = node * CORES + core
    peers = [lax.rem(me + by, M * CORES) for by in range(1, M * CORES)]
    swap(st3, me, sums, [(dev(chip, lax.rem(p, CORES)), lax.div(p, CORES)) for p in peers], s3s, s3r)
    sums = st3[0]
    for slot in range(1, M * CORES):
        sums = sums + st3[slot]
    sums_ref[...] = sums

    def ended(flow, count):
        view = own.at[:, cols(0, count)]
        pltpu.make_async_copy(view, view, zsend.at[flow]).wait()

    ended(4, 2 + TILE * (sets - 2))

    @pl.when(has_next)
    def _():
        ended(0, 2 + TILE * (sets - 2))
        ended(1, 2 + TILE * (sets - 2))

    @pl.when(far_source)
    def _():
        for which in range(CORES):
            ended(2 + which, 2 + TILE * (sets - 2))

    @pl.when(far_middle)
    def _():
        for which in range(CORES):
            ended(5 + which, 2 + TILE * (sets - 2))

    made = arena.at[OUT, :, cols(0, half)]

    def drained(sem):
        pltpu.make_async_copy(made, made, sem).wait()

    for away in range(M):
        for which in range(CORES):
            drained(osend.at[which, away])
            if away:
                drained(orecv.at[which, away])
    drained(orecv.at[1 - core, 0])


def finish(mean_count, made_ref, sums_ref, out_ref, log_ref, row, sem):
    systems = made_ref.shape[2]
    flows = []
    for block in range(systems // ROWS):
        rows = pl.ds(block * ROWS, ROWS)
        flows.append(pltpu.make_async_copy(made_ref.at[0, 0, rows], out_ref.at[0, 0, rows], sem.at[block]))
    for c in flows:
        c.start()
    row[...] = jnp.log(log_floor + sums_ref[...] / mean_count)[:SWEEPS, :systems]
    last = pltpu.make_async_copy(row, log_ref, sem.at[systems // ROWS])
    last.start()
    for c in flows:
        c.wait()
    last.wait()


def body(sizes, slice_starts, coupling):
    systems, cells = coupling.shape
    ny, nz = sizes
    half = cells // LANES // CORES
    tiles = half // TILE
    span = half + 2 * TILE + 6
    mean_count = float(ny * nz * CORES * M * cells)
    flat = lambda *lead: pltpu.VMEM(lead + (ROWS, span * LANES), jnp.float32)
    dma = pltpu.SemaphoreType.DMA
    any_spec = pl.BlockSpec(memory_space=pl.ANY)
    out = jax.ShapeDtypeStruct((1, 1, systems, cells), jnp.float32)
    made, sums = pl.pallas_call(
        functools.partial(kernel, (ny, nz, cells)),
        out_shape=(out, jax.ShapeDtypeStruct((ROWS, LANES), jnp.float32)),
        in_specs=[pl.BlockSpec(memory_space=pltpu.HBM)] * 2,
        out_specs=(any_spec, pl.BlockSpec(memory_space=pltpu.VMEM)),
        scratch_shapes=[
            pltpu.VMEM((ROWS, cells), jnp.float32), flat(CORES), flat(PLACES),
            pltpu.VMEM((SWEEPS, ROWS, LANES), jnp.float32),
            pltpu.VMEM((nz, ROWS, LANES), jnp.float32),
            pltpu.VMEM((ny, ROWS, LANES), jnp.float32),
            pltpu.VMEM((M * CORES, ROWS, LANES), jnp.float32),
            dma((1,)), dma((tiles + 2,)), dma((5, tiles + 2)), dma((CORES, tiles + 2)), dma((7,)),
            dma((CORES, M)), dma((CORES, M)),
            dma((nz,)), dma((nz,)), dma((ny,)), dma((ny,)), dma((M * CORES,)), dma((M * CORES,)),
        ],
        compiler_params=pltpu.CompilerParams(
            collective_id=0, has_side_effects=True, vmem_limit_bytes=51 * 2**20
        ),
        name="sdc",
    )(slice_starts, coupling)
    return pl.pallas_call(
        functools.partial(finish, mean_count),
        out_shape=(out, jax.ShapeDtypeStruct((SWEEPS, systems), jnp.float32)),
        in_specs=[any_spec, pl.BlockSpec(memory_space=pltpu.VMEM)],
        out_specs=(pl.BlockSpec(memory_space=pltpu.HBM),) * 2,
        scratch_shapes=[pltpu.VMEM((SWEEPS, systems), jnp.float32), dma((systems // ROWS + 1,))],
        compiler_params=pltpu.CompilerParams(vmem_limit_bytes=2**20),
        name="finish",
    )(made, sums)


def solution(mesh):
    chips = mesh.shape["tm"] // CORES
    ny = 4
    return jax.shard_map(
        functools.partial(body, (ny, chips // ny)),
        mesh=mesh,
        in_specs=(P("tm", None, None), P()),
        out_specs=(P("tm", "node", None, None), P()),
        check_vma=False,
    )
```

```python
import functools

import jax
import jax.numpy as jnp
import numpy as np
from jax import lax
from jax.experimental import pallas as pl
from jax.experimental.pallas import tpu as pltpu
from jax.sharding import PartitionSpec as P

M = 4
SWEEPS = 3
CORES = 2
LANES = 128
ROWS = 8
SUB = 2
TILE = 4
PAD = TILE + 1
time_step = 0.5
log_floor = 0.05


def legendre_gap(point, node_count):
    before = 1.0
    current = point
    for degree in range(1, node_count):
        following = ((2 * degree + 1) * point * current - degree * before) / (degree + 1)
        before = current
        current = following
    return current - before


def collocation(node_count):
    points = []
    samples = 4000
    for sample_index in range(samples - 1):
        lower_end = -1.0 + 2.0 * sample_index / samples
        upper_end = -1.0 + 2.0 * (sample_index + 1) / samples
        lower_value = legendre_gap(lower_end, node_count)
        upper_value = legendre_gap(upper_end, node_count)
        if lower_value * upper_value < 0.0:
            for halving in range(80):
                middle = 0.5 * (lower_end + upper_end)
                middle_value = legendre_gap(middle, node_count)
                if lower_value * middle_value <= 0.0:
                    upper_end = middle
                else:
                    lower_end = middle
                    lower_value = middle_value
            points.append(0.5 * (lower_end + upper_end))
    points.append(1.0)
    node_times = [(point + 1.0) / 2.0 for point in points]
    matrix = [[0.0] * node_count for row_index in range(node_count)]
    for column in range(node_count):
        coeffs = [1.0]
        for other in range(node_count):
            if other != column:
                scale = node_times[column] - node_times[other]
                shifted = [0.0] + coeffs
                scaled = [value * node_times[other] for value in coeffs] + [0.0]
                coeffs = [(shifted[power] - scaled[power]) / scale for power in range(len(shifted))]
        for row_index in range(node_count):
            upper_time = node_times[row_index]
            matrix[row_index][column] = sum(
                coeffs[power] * upper_time ** (power + 1) / (power + 1) for power in range(len(coeffs))
            )
    return (node_times, matrix)


NODE_TIMES, MATRIX = collocation(M)
WEIGHTS = [[time_step * float(np.float32(q)) for q in row] for row in MATRIX]
IMPLICIT = [float(np.float32(time_step * t / M)) for t in NODE_TIMES]
ROW_SUMS = [sum(row) for row in WEIGHTS]


LAG = 3
AHEAD = 3


SS = 0
CP, CL, CS = 5, 6, 7
U1 = 8
E1 = U1 + 3 * M * 3
U2 = E1 + 1
E2 = U2 + 2 * M * 3
OUT = E2 + 1
PLACES = OUT + 2 * M


def kernel(sizes, ss_ref, cp_ref, out_ref, sums_ref, own, transit, arena, acc, st1, st2,
           wsem, csem, rsem, tsem, zsend, osend, orecv, s1s, s1r, s2s, s2r, met):
    ny, nz, cells = sizes
    half = cells // LANES // CORES
    tiles = half // TILE
    whole = cells // LANES
    chips = ny * nz
    sets = tiles + 2
    tm = lax.axis_index("tm")
    node = lax.axis_index("node")
    core = lax.rem(tm, CORES)
    chip = lax.div(tm, CORES)
    zpos = lax.rem(chip, nz)
    ypos = lax.div(chip, nz)
    rows = pl.ds(pl.multiple_of(node * ROWS, ROWS), ROWS)

    middle = jnp.where(zpos == 0, chip + nz - 1, chip - 1)
    source_chip = jnp.where(zpos == nz - 1, chip - nz + 1, chip + 1)
    target = jnp.where(zpos == nz - 1, chip - 1, chip + nz - 1)
    middle_of_target = jnp.where(zpos == 2, chip + 1, chip - nz + 1)
    has_next = chip < chips - 1
    has_before = chip > 0
    far_source = jnp.logical_and(core == 1, chip < chips - 2)
    far_target = chip > 1
    is_middle = source_chip < chips - 2
    far_middle = jnp.logical_and(core == 0, is_middle)

    def dev(which_chip, which):
        return which_chip * CORES + which

    def cols(start, count):
        if isinstance(start, int):
            return pl.ds(start * LANES, count * LANES)
        return pl.ds(pl.multiple_of(start * LANES, LANES), count * LANES)

    def remote(src, dst, send, recv, to_tm, to_node):
        return pltpu.make_async_remote_copy(
            src, dst, send, recv, device_id=(to_tm, to_node), device_id_type=pl.DeviceIdType.MESH
        )

    def source(which, a):
        if isinstance(a, int) and a == 0:
            return lax.rem(half * which + whole - 1, whole), PAD - 1, 1
        count = 1 if isinstance(a, int) and a == sets - 1 else TILE
        return lax.rem(half * which + TILE * (a - 1), whole), PAD + TILE * (a - 1), count

    def each_set(a, what):
        pl.when(a < sets - 1)(lambda: what(a))
        pl.when(a == sets - 1)(lambda: what(sets - 1))

    def local_set(a):
        start, q, count = source(core, a)
        pltpu.make_async_copy(cp_ref.at[rows, cols(start, count)], arena.at[CP, :, cols(q, count)], csem.at[a]).start()
        pltpu.make_async_copy(
            ss_ref.at[0, rows, cols(start, count)], arena.at[3 + core, :, cols(q, count)], rsem.at[3 + core, a]
        ).start()

    def near_set(a):
        @pl.when(has_next)
        def _():
            for which in range(CORES):
                start, q, count = source(which, a)
                remote(own.at[:, cols(start, count)], arena.at[1 + core, :, cols(q, count)],
                       zsend.at[which], rsem.at[1 + core, a], dev(chip + 1, which), node).start()

        start, q, count = source(1 - core, a)
        remote(own.at[:, cols(start, count)], arena.at[3 + core, :, cols(q, count)],
               zsend.at[4], rsem.at[3 + core, a], dev(chip, 1 - core), node).start()

    def first_leg(a):
        @pl.when(far_source)
        def _():
            for which in range(CORES):
                start, q, count = source(which, a)
                remote(own.at[:, cols(start, count)], transit.at[which, :, cols(q, count)],
                       zsend.at[2 + which], tsem.at[which, a], dev(middle, 0), node).start()

    def second_leg(a):
        for which in range(CORES):
            _, q, count = source(which, a)
            view = transit.at[which, :, cols(q, count)]
            pltpu.make_async_copy(view, view, tsem.at[which, a]).wait()
            remote(view, arena.at[0, :, cols(q, count)],
                   zsend.at[5 + which], rsem.at[0, a], dev(target, which), node).start()

    def wait_set(a):
        _, q, count = source(core, a)
        pltpu.make_async_copy(arena.at[CP, :, cols(q, count)], arena.at[CP, :, cols(q, count)], csem.at[a]).wait()

        def arrived(n):
            view = arena.at[n, :, cols(q, count)]
            pltpu.make_async_copy(view, view, rsem.at[n, a]).wait()

        arrived(3)
        arrived(4)

        @pl.when(has_before)
        def _():
            arrived(1)
            arrived(2)

    def wait_far_set(a):
        @pl.when(far_target)
        def _():
            _, q, count = source(core, a)
            view = arena.at[0, :, cols(q, count)]
            pltpu.make_async_copy(view, view, rsem.at[0, a]).wait()

    barrier = pltpu.get_barrier_semaphore()

    def greet(to_tm, to_node):
        pl.semaphore_signal(barrier, inc=1, device_id=(to_tm, to_node), device_id_type=pl.DeviceIdType.MESH)

    def both(which_chip):
        for which in range(CORES):
            greet(dev(which_chip, which), node)

    greeted = jnp.int32(0)
    for cond, count, hello in (
        (has_next, 2, lambda: both(chip + 1)),
        (has_before, 2, lambda: both(chip - 1)),
        (far_source, 1, lambda: greet(dev(middle, 0), node)),
        (far_middle, 1, lambda: greet(dev(source_chip, 1), node)),
        (far_middle, 2, lambda: both(target)),
        (far_target, 1, lambda: greet(dev(middle_of_target, 0), node)),
    ):
        pl.when(cond)(hello)
        greeted = greeted + jnp.where(cond, count, 0)
    greet(dev(chip, 1 - core), node)
    for by in range(1, M):
        for which in range(CORES):
            greet(dev(chip, which), lax.rem(node + by, M))
    for by in range(1, nz):
        greet(dev(ypos * nz + lax.rem(zpos + by, nz), core), node)
    for by in range(1, ny):
        greet(dev(lax.rem(ypos + by, ny) * nz + zpos, core), node)
    always = CORES * M - 1 + nz - 1 + ny - 1
    fetch = pltpu.make_async_copy(ss_ref.at[0, rows, :], own, wsem.at[0])
    fetch.start()
    local_set(0)

    @pl.loop(1, sets - 1)
    def _(a):
        local_set(a)

    local_set(sets - 1)

    pl.semaphore_wait(barrier, greeted + always)
    fetch.wait()

    near_set(0)
    first_leg(0)

    @pl.loop(1, sets - 1)
    def _(a):
        near_set(a)
        first_leg(a)

    near_set(sets - 1)
    first_leg(sets - 1)

    for by in range(1, ny):
        pl.semaphore_signal(met, inc=1, device_id=(dev(lax.rem(ypos + by, ny) * nz + zpos, core), node),
                            device_id_type=pl.DeviceIdType.MESH)
    acc[...] = jnp.zeros_like(acc)
    first = chip == 0
    second = chip == 1
    width = SUB * LANES
    lane = lax.broadcasted_iota(jnp.int32, (ROWS, width), 1) % LANES
    low = lane == 0
    high = lane == LANES - 1

    def load(v, place, q, count=SUB):
        return v[place, :, cols(q, count)]

    def piece(value, t):
        return value[:, t * LANES:(t + 1) * LANES]

    def rolled(v, place, q, count, by):
        return jnp.concatenate([pltpu.roll(load(v, place, q + t, 1), by, axis=1) for t in range(count)], axis=1)

    def pick_right(turned):
        return jnp.where(high, turned[:, LANES:], turned[:, :width])

    def pick_left(turned):
        return jnp.where(low, turned[:, :width], turned[:, LANES:])

    def force(u, square, right, left, parts):
        c, cl, cs = parts
        return c * right + cl * left + u * (cs - square)

    def newton(u, square3, defect, target, m):
        a = IMPLICIT[m]
        once = u + defect / ((1.0 - a) + square3)
        square = once * once
        return (target + (2.0 * a) * square * once) / ((1.0 - a) + (3.0 * a) * square)

    def keep(v, place, q, new):
        for t in range(SUB):
            part = piece(new, t)
            v[place, :, cols(q + t, 1)] = part
            v[place + 1, :, cols(q + t, 1)] = pltpu.roll(part, LANES - 1, axis=1)
            v[place + 2, :, cols(q + t, 1)] = pltpu.roll(part, 1, axis=1)

    def add_up(k, q, total):
        whole_tile = None
        for t in range(SUB):
            mine = jnp.logical_and(q + t >= PAD, q + t < PAD + half)
            part = jnp.where(mine, piece(total, t), jnp.zeros((ROWS, LANES), jnp.float32))
            whole_tile = part if whole_tile is None else whole_tile + part
        acc[k] += whole_tile

    def start_sweep(v, first_col, q, slices):
        here = cols(q, SUB)
        c = load(v, CP, q)
        if 1 in slices:
            parts = (c, load(v, CL, q), load(v, CS, q))
        else:
            cl = pick_left(rolled(v, CP, q - 1, SUB + 1, 1))
            cs = 1.0 - (c + cl)
            v[CL, :, here] = cl
            v[CS, :, here] = cs
            parts = (c, cl, cs)
        total = None
        for n in slices:
            u = load(v, SS + n, q)
            square = u * u
            f = force(u, square, pick_right(rolled(v, SS + n, q, SUB + 1, LANES - 1)),
                      pick_left(rolled(v, SS + n, q - 1, SUB + 1, 1)), parts)
            before = load(v, SS + n - 1, q)
            if n == 3:
                before = jnp.where(first, u, before)
            if n == 1:
                before = jnp.where(second, u, before)
            pull = f - 0.25 * (u - u * square)
            gap = before - u
            for m in range(M):
                if n == 1 and m < M - 1:
                    continue
                defect = gap + ROW_SUMS[m] * f
                new = newton(u, (3.0 * IMPLICIT[m]) * square, defect, before + ROW_SUMS[m] * pull, m)
                if n == 1:
                    v[E1, :, here] = new
                else:
                    keep(v, U1 + ((n - 2) * M + m) * 3, q, new)
                if n >= 3:
                    total = defect * defect if total is None else total + defect * defect
        if total is not None:
            add_up(0, first_col + q, total)

    def later_sweep(v, first_col, k, q, slices):
        here = cols(q, SUB)
        parts = (load(v, CP, q), load(v, CL, q), load(v, CS, q))
        total = None
        for n in slices:
            at = U1 + (n - 2) * M * 3 if k == 1 else U2 + (n - 3) * M * 3
            us, squares, forces = [], [], []
            for m in range(M):
                u = load(v, at + 3 * m, q)
                square = u * u
                right = pick_right(load(v, at + 3 * m + 1, q, SUB + 1))
                left = pick_left(load(v, at + 3 * m + 2, q - 1, SUB + 1))
                us.append(u)
                squares.append(square)
                forces.append(force(u, square, right, left, parts))
            if n == 2:
                before = load(v, E1, q)
            elif n == 3:
                before = load(v, U1 + (M - 1) * 3 if k == 1 else E2, q)
                before = jnp.where(first, load(v, SS + 3, q), before)
            else:
                before = load(v, at - 3, q)
            for m in range(M):
                if n == 2 and m < M - 1:
                    continue
                base = before
                for j in range(M):
                    base = base + WEIGHTS[m][j] * forces[j]
                a = IMPLICIT[m]
                defect = base - us[m]
                scaled = a * squares[m]
                target = defect + us[m] * ((1.0 - a) + scaled)
                new = newton(us[m], 3.0 * scaled, defect, target, m)
                if n == 2:
                    v[E2, :, here] = new
                elif k == 1:
                    keep(v, U2 + ((n - 3) * M + m) * 3, q, new)
                else:
                    v[OUT + (n - 3) * M + m, :, here] = new
                if n >= 3:
                    total = defect * defect if total is None else total + defect * defect
        if total is not None:
            add_up(k, first_col + q, total)

    def window(step):
        return arena.at[:, :, cols(step * TILE, TILE + 6)], step * TILE

    def main_part(step):
        v, at = window(step)
        for g in range(0, TILE, SUB):
            start_sweep(v, at, 3 + g, (4, 3, 2))
        for g in range(0, TILE, SUB):
            later_sweep(v, at, 1, 2 + g, (4, 3))
        for g in range(0, TILE, SUB):
            later_sweep(v, at, 2, 1 + g, (4,))

    def lagging_part(step):
        v, at = window(step)
        for g in range(0, TILE, SUB):
            start_sweep(v, at, 3 + g, (1,))
        for g in range(0, TILE, SUB):
            later_sweep(v, at, 1, 2 + g, (2,))
        for g in range(0, TILE, SUB):
            later_sweep(v, at, 2, 1 + g, (3,))

    def send_out(which, i):
        place = cols(core * half + TILE * i, TILE)
        for away in range(M):
            to_node = lax.rem(node + away, M)
            src = arena.at[OUT + which * M + to_node, :, cols(PAD + TILE * i, TILE)]
            dst = out_ref.at[0, 0, rows, place]
            out = remote(src, dst, osend.at[which, away], orecv.at[core, away], dev(chip, which), to_node)
            if away:
                out.start()
            else:
                pl.when(core != which)(out.start)
                pl.when(core == which)(pltpu.make_async_copy(src, dst, osend.at[which, 0]).start)

    wait_set(0)

    @pl.when(far_middle)
    def _():
        second_leg(0)

        @pl.loop(1, AHEAD)
        def _(a):
            second_leg(a)

    wait_far_set(0)

    @pl.loop(0, tiles + 1 + LAG)
    def _(step):
        @pl.when(far_middle)
        def _():
            each_set(step + AHEAD, second_leg)

        @pl.when(step <= tiles)
        def _():
            i = step - 1
            each_set(step + 1, wait_set)
            main_part(step)
            pl.when(i >= 0)(lambda: send_out(1, i))

        @pl.when(step >= LAG)
        def _():
            i = step - 1 - LAG
            each_set(i + 2, wait_far_set)
            lagging_part(step - LAG)
            pl.when(i >= 0)(lambda: send_out(0, i))

    row = lax.broadcasted_iota(jnp.int32, (ROWS, LANES), 0)
    column = lax.broadcasted_iota(jnp.int32, (ROWS, LANES), 1)
    place = column == node * ROWS + row
    sums = jnp.zeros((ROWS, LANES), jnp.float32)
    for k in range(SWEEPS):
        spread = jnp.where(place, jnp.sum(acc[k], axis=1, keepdims=True), 0.0)
        sums = jnp.where(row == k, jnp.sum(spread, axis=0, keepdims=True), sums)

    def swap(store, mine, value, peers, send, recv):
        store[mine] = value
        flows = [
            remote(store.at[mine], store.at[mine], send.at[by], recv.at[by], to_tm, to_node)
            for by, (to_tm, to_node) in enumerate(peers)
        ]
        for c in flows:
            c.start()
        for c in flows:
            c.wait()

    pl.semaphore_wait(met, ny - 1)
    others = [lax.rem(ypos + by, ny) * nz + lax.rem(zpos + bz, nz) for by in range(ny) for bz in range(nz) if by or bz]
    swap(st1, chip, sums, [(dev(c, core), node) for c in others], s1s, s1r)
    sums = st1[0]
    for slot in range(1, chips):
        sums = sums + st1[slot]
    me = node * CORES + core
    peers = [lax.rem(me + by, M * CORES) for by in range(1, M * CORES)]
    swap(st2, me, sums, [(dev(chip, lax.rem(p, CORES)), lax.div(p, CORES)) for p in peers], s2s, s2r)
    sums = st2[0]
    for slot in range(1, M * CORES):
        sums = sums + st2[slot]
    sums_ref[...] = sums

    def ended(flow, count):
        view = own.at[:, cols(0, count)]
        pltpu.make_async_copy(view, view, zsend.at[flow]).wait()

    ended(4, 2 + TILE * (sets - 2))

    @pl.when(has_next)
    def _():
        ended(0, 2 + TILE * (sets - 2))
        ended(1, 2 + TILE * (sets - 2))

    @pl.when(far_source)
    def _():
        for which in range(CORES):
            ended(2 + which, 2 + TILE * (sets - 2))

    @pl.when(far_middle)
    def _():
        for which in range(CORES):
            ended(5 + which, 2 + TILE * (sets - 2))

    made = arena.at[OUT, :, cols(0, half)]

    def drained(sem):
        pltpu.make_async_copy(made, made, sem).wait()

    for away in range(M):
        for which in range(CORES):
            drained(osend.at[which, away])
            if away:
                drained(orecv.at[which, away])
    drained(orecv.at[1 - core, 0])


def finish(mean_count, made_ref, sums_ref, out_ref, log_ref, row, sem):
    systems = made_ref.shape[2]
    flows = []
    for block in range(systems // ROWS):
        rows = pl.ds(block * ROWS, ROWS)
        flows.append(pltpu.make_async_copy(made_ref.at[0, 0, rows], out_ref.at[0, 0, rows], sem.at[block]))
    for c in flows:
        c.start()
    row[...] = jnp.log(log_floor + sums_ref[...] / mean_count)[:SWEEPS, :systems]
    last = pltpu.make_async_copy(row, log_ref, sem.at[systems // ROWS])
    last.start()
    for c in flows:
        c.wait()
    last.wait()


def body(sizes, slice_starts, coupling):
    systems, cells = coupling.shape
    ny, nz = sizes
    half = cells // LANES // CORES
    tiles = half // TILE
    span = half + 2 * TILE + 6
    mean_count = float(ny * nz * CORES * M * cells)
    flat = lambda *lead: pltpu.VMEM(lead + (ROWS, span * LANES), jnp.float32)
    dma = pltpu.SemaphoreType.DMA
    any_spec = pl.BlockSpec(memory_space=pl.ANY)
    out = jax.ShapeDtypeStruct((1, 1, systems, cells), jnp.float32)
    made, sums = pl.pallas_call(
        functools.partial(kernel, (ny, nz, cells)),
        out_shape=(out, jax.ShapeDtypeStruct((ROWS, LANES), jnp.float32)),
        in_specs=[pl.BlockSpec(memory_space=pltpu.HBM)] * 2,
        out_specs=(any_spec, pl.BlockSpec(memory_space=pltpu.VMEM)),
        scratch_shapes=[
            pltpu.VMEM((ROWS, cells), jnp.float32), flat(CORES), flat(PLACES),
            pltpu.VMEM((SWEEPS, ROWS, LANES), jnp.float32),
            pltpu.VMEM((ny * nz, ROWS, LANES), jnp.float32),
            pltpu.VMEM((M * CORES, ROWS, LANES), jnp.float32),
            dma((1,)), dma((tiles + 2,)), dma((5, tiles + 2)), dma((CORES, tiles + 2)), dma((7,)),
            dma((CORES, M)), dma((CORES, M)),
            dma((ny * nz,)), dma((ny * nz,)), dma((M * CORES,)), dma((M * CORES,)),
            pltpu.SemaphoreType.REGULAR,
        ],
        compiler_params=pltpu.CompilerParams(
            collective_id=0, has_side_effects=True, vmem_limit_bytes=51 * 2**20
        ),
        name="sdc",
    )(slice_starts, coupling)
    return pl.pallas_call(
        functools.partial(finish, mean_count),
        out_shape=(out, jax.ShapeDtypeStruct((SWEEPS, systems), jnp.float32)),
        in_specs=[any_spec, pl.BlockSpec(memory_space=pltpu.VMEM)],
        out_specs=(pl.BlockSpec(memory_space=pltpu.HBM),) * 2,
        scratch_shapes=[pltpu.VMEM((SWEEPS, systems), jnp.float32), dma((systems // ROWS + 1,))],
        compiler_params=pltpu.CompilerParams(vmem_limit_bytes=2**20),
        name="finish",
    )(made, sums)


def solution(mesh):
    chips = mesh.shape["tm"] // CORES
    ny = 4
    return jax.shard_map(
        functools.partial(body, (ny, chips // ny)),
        mesh=mesh,
        in_specs=(P("tm", None, None), P()),
        out_specs=(P("tm", "node", None, None), P()),
        check_vma=False,
    )
```

```python
import functools

import jax
import jax.numpy as jnp
import numpy as np
from jax import lax
from jax.experimental import pallas as pl
from jax.experimental.pallas import tpu as pltpu
from jax.sharding import PartitionSpec as P

M = 4
SWEEPS = 3
CORES = 2
LANES = 128
ROWS = 8
SUB = 2
TILE = 4
PAD = TILE + 1
time_step = 0.5
log_floor = 0.05


def legendre_gap(point, node_count):
    before = 1.0
    current = point
    for degree in range(1, node_count):
        following = ((2 * degree + 1) * point * current - degree * before) / (degree + 1)
        before = current
        current = following
    return current - before


def collocation(node_count):
    points = []
    samples = 4000
    for sample_index in range(samples - 1):
        lower_end = -1.0 + 2.0 * sample_index / samples
        upper_end = -1.0 + 2.0 * (sample_index + 1) / samples
        lower_value = legendre_gap(lower_end, node_count)
        upper_value = legendre_gap(upper_end, node_count)
        if lower_value * upper_value < 0.0:
            for halving in range(80):
                middle = 0.5 * (lower_end + upper_end)
                middle_value = legendre_gap(middle, node_count)
                if lower_value * middle_value <= 0.0:
                    upper_end = middle
                else:
                    lower_end = middle
                    lower_value = middle_value
            points.append(0.5 * (lower_end + upper_end))
    points.append(1.0)
    node_times = [(point + 1.0) / 2.0 for point in points]
    matrix = [[0.0] * node_count for row_index in range(node_count)]
    for column in range(node_count):
        coeffs = [1.0]
        for other in range(node_count):
            if other != column:
                scale = node_times[column] - node_times[other]
                shifted = [0.0] + coeffs
                scaled = [value * node_times[other] for value in coeffs] + [0.0]
                coeffs = [(shifted[power] - scaled[power]) / scale for power in range(len(shifted))]
        for row_index in range(node_count):
            upper_time = node_times[row_index]
            matrix[row_index][column] = sum(
                coeffs[power] * upper_time ** (power + 1) / (power + 1) for power in range(len(coeffs))
            )
    return (node_times, matrix)


NODE_TIMES, MATRIX = collocation(M)
WEIGHTS = [[time_step * float(np.float32(q)) for q in row] for row in MATRIX]
IMPLICIT = [float(np.float32(time_step * t / M)) for t in NODE_TIMES]
ROW_SUMS = [sum(row) for row in WEIGHTS]


LAG = 3
MIX = 16
AHEAD = 3


SS = 0
CP, CL, CS = 5, 6, 7
U1 = 8
E1 = U1 + 3 * M * 3
U2 = E1 + 1
E2 = U2 + 2 * M * 3
OUT = E2 + 1
PLACES = OUT + 2 * M


def kernel(sizes, ss_ref, cp_ref, out_ref, sums_ref, own, transit, arena, acc, st1, st2,
           wsem, csem, rsem, tsem, zsend, osend, orecv, s1s, s1r, s2s, s2r, met):
    ny, nz, cells = sizes
    half = cells // LANES // CORES
    tiles = half // TILE
    whole = cells // LANES
    chips = ny * nz
    main_sets = tiles + 2
    sets = main_sets + MIX // TILE + 2
    single = (0, main_sets - 1, main_sets, sets - 1)
    second_window = tiles + 3
    second_pad = PAD + second_window * TILE
    tm = lax.axis_index("tm")
    node = lax.axis_index("node")
    core = lax.rem(tm, CORES)
    chip = lax.div(tm, CORES)
    zpos = lax.rem(chip, nz)
    ypos = lax.div(chip, nz)
    blocks = (node, lax.rem(node + 2, M))
    rows = [pl.ds(pl.multiple_of(b * ROWS, ROWS), ROWS) for b in blocks]

    middle = jnp.where(zpos == 0, chip + nz - 1, chip - 1)
    source_chip = jnp.where(zpos == nz - 1, chip - nz + 1, chip + 1)
    target = jnp.where(zpos == nz - 1, chip - 1, chip + nz - 1)
    middle_of_target = jnp.where(zpos == 2, chip + 1, chip - nz + 1)
    has_next = chip < chips - 1
    has_before = chip > 0
    far_source = jnp.logical_and(core == 1, chip < chips - 2)
    far_target = chip > 1
    is_middle = source_chip < chips - 2
    far_middle = jnp.logical_and(core == 0, is_middle)

    def dev(which_chip, which):
        return which_chip * CORES + which

    def cols(start, count):
        if isinstance(start, int):
            return pl.ds(start * LANES, count * LANES)
        return pl.ds(pl.multiple_of(start * LANES, LANES), count * LANES)

    def remote(src, dst, send, recv, to_tm, to_node):
        return pltpu.make_async_remote_copy(
            src, dst, send, recv, device_id=(to_tm, to_node), device_id_type=pl.DeviceIdType.MESH
        )

    def source(which, a, part=0):
        if isinstance(a, int):
            part = 1 if a >= main_sets else 0
        b = a - part * main_sets
        j = -1 if isinstance(b, int) and b == 0 else TILE * (b - 1)
        first_column = half * which + (half - MIX if part else 0)
        count = 1 if isinstance(a, int) and a in single else TILE
        return part, lax.rem(first_column + j + whole, whole), (second_pad if part else PAD) + j, count

    def each_set(a, what):
        pl.when(a < main_sets - 1)(lambda: what(a))
        pl.when(a == main_sets - 1)(lambda: what(main_sets - 1))

    def in_turn(what):
        what(0)
        pl.loop(1, main_sets - 1)(lambda a: what(a))
        what(main_sets - 1)
        what(main_sets)
        pl.loop(main_sets + 1, sets - 1)(lambda a: what(a, 1))
        what(sets - 1)

    def local_set(a, part=0):
        part, start, q, count = source(core, a, part)
        pltpu.make_async_copy(
            cp_ref.at[rows[part], cols(start, count)], arena.at[CP, :, cols(q, count)], csem.at[a]
        ).start()
        pltpu.make_async_copy(
            ss_ref.at[0, rows[part], cols(start, count)], arena.at[3 + core, :, cols(q, count)], rsem.at[3 + core, a]
        ).start()

    def near_set(a, part=0):
        @pl.when(has_next)
        def _():
            for which in range(CORES):
                p, start, q, count = source(which, a, part)
                remote(own.at[p, :, cols(start, count)], arena.at[1 + core, :, cols(q, count)],
                       zsend.at[which], rsem.at[1 + core, a], dev(chip + 1, which), node).start()

        p, start, q, count = source(1 - core, a, part)
        remote(own.at[p, :, cols(start, count)], arena.at[3 + core, :, cols(q, count)],
               zsend.at[4], rsem.at[3 + core, a], dev(chip, 1 - core), node).start()

    def first_leg(a, part=0):
        @pl.when(far_source)
        def _():
            for which in range(CORES):
                p, start, q, count = source(which, a, part)
                remote(own.at[p, :, cols(start, count)], transit.at[which, :, cols(q, count)],
                       zsend.at[2 + which], tsem.at[which, a], dev(middle, 0), node).start()

    def near_and_leg(a, part=0):
        near_set(a, part)
        first_leg(a, part)

    def second_leg(a, part=0):
        for which in range(CORES):
            _, _, q, count = source(which, a, part)
            view = transit.at[which, :, cols(q, count)]
            pltpu.make_async_copy(view, view, tsem.at[which, a]).wait()
            remote(view, arena.at[0, :, cols(q, count)],
                   zsend.at[5 + which], rsem.at[0, a], dev(target, which), node).start()

    def wait_set(a, part=0):
        _, _, q, count = source(core, a, part)
        pltpu.make_async_copy(arena.at[CP, :, cols(q, count)], arena.at[CP, :, cols(q, count)], csem.at[a]).wait()

        def arrived(n):
            view = arena.at[n, :, cols(q, count)]
            pltpu.make_async_copy(view, view, rsem.at[n, a]).wait()

        arrived(3)
        arrived(4)

        @pl.when(has_before)
        def _():
            arrived(1)
            arrived(2)

    def wait_far_set(a, part=0):
        @pl.when(far_target)
        def _():
            _, _, q, count = source(core, a, part)
            view = arena.at[0, :, cols(q, count)]
            pltpu.make_async_copy(view, view, rsem.at[0, a]).wait()

    barrier = pltpu.get_barrier_semaphore()

    def greet(to_tm, to_node):
        pl.semaphore_signal(barrier, inc=1, device_id=(to_tm, to_node), device_id_type=pl.DeviceIdType.MESH)

    def both(which_chip):
        for which in range(CORES):
            greet(dev(which_chip, which), node)

    greeted = jnp.int32(0)
    for cond, count, hello in (
        (has_next, 2, lambda: both(chip + 1)),
        (has_before, 2, lambda: both(chip - 1)),
        (far_source, 1, lambda: greet(dev(middle, 0), node)),
        (far_middle, 1, lambda: greet(dev(source_chip, 1), node)),
        (far_middle, 2, lambda: both(target)),
        (far_target, 1, lambda: greet(dev(middle_of_target, 0), node)),
    ):
        pl.when(cond)(hello)
        greeted = greeted + jnp.where(cond, count, 0)
    greet(dev(chip, 1 - core), node)
    for by in range(1, M):
        for which in range(CORES):
            greet(dev(chip, which), lax.rem(node + by, M))
    for by in range(1, nz):
        greet(dev(ypos * nz + lax.rem(zpos + by, nz), core), node)
    for by in range(1, ny):
        greet(dev(lax.rem(ypos + by, ny) * nz + zpos, core), node)
    always = CORES * M - 1 + nz - 1 + ny - 1
    fetches = [pltpu.make_async_copy(ss_ref.at[0, rows[p], :], own.at[p], wsem.at[p]) for p in range(2)]
    for fetch in fetches:
        fetch.start()
    in_turn(local_set)

    pl.semaphore_wait(barrier, greeted + always)
    for fetch in fetches:
        fetch.wait()
    in_turn(near_and_leg)

    for by in range(1, ny):
        pl.semaphore_signal(met, inc=1, device_id=(dev(lax.rem(ypos + by, ny) * nz + zpos, core), node),
                            device_id_type=pl.DeviceIdType.MESH)
    acc[...] = jnp.zeros_like(acc)
    first = chip == 0
    second = chip == 1
    width = SUB * LANES
    lane = lax.broadcasted_iota(jnp.int32, (ROWS, width), 1) % LANES
    low = lane == 0
    high = lane == LANES - 1

    def load(v, place, q, count=SUB):
        return v[place, :, cols(q, count)]

    def piece(value, t):
        return value[:, t * LANES:(t + 1) * LANES]

    def rolled(v, place, q, count, by):
        return jnp.concatenate([pltpu.roll(load(v, place, q + t, 1), by, axis=1) for t in range(count)], axis=1)

    def pick_right(turned):
        return jnp.where(high, turned[:, LANES:], turned[:, :width])

    def pick_left(turned):
        return jnp.where(low, turned[:, :width], turned[:, LANES:])

    def force(u, square, right, left, parts):
        c, cl, cs = parts
        return c * right + cl * left + u * (cs - square)

    def newton(u, square3, defect, target, m):
        a = IMPLICIT[m]
        once = u + defect / ((1.0 - a) + square3)
        square = once * once
        return (target + (2.0 * a) * square * once) / ((1.0 - a) + (3.0 * a) * square)

    def keep(v, place, q, new):
        for t in range(SUB):
            part = piece(new, t)
            v[place, :, cols(q + t, 1)] = part
            v[place + 1, :, cols(q + t, 1)] = pltpu.roll(part, LANES - 1, axis=1)
            v[place + 2, :, cols(q + t, 1)] = pltpu.roll(part, 1, axis=1)

    def add_up(k, q, total):
        whole_tile = None
        for t in range(SUB):
            mine = jnp.logical_and(q + t >= PAD, q + t < PAD + half)
            part = jnp.where(mine, piece(total, t), jnp.zeros((ROWS, LANES), jnp.float32))
            whole_tile = part if whole_tile is None else whole_tile + part
        acc[k] += whole_tile

    def start_sweep(v, first_col, q, slices, counted):
        here = cols(q, SUB)
        c = load(v, CP, q)
        if 1 in slices:
            parts = (c, load(v, CL, q), load(v, CS, q))
        else:
            cl = pick_left(rolled(v, CP, q - 1, SUB + 1, 1))
            cs = 1.0 - (c + cl)
            v[CL, :, here] = cl
            v[CS, :, here] = cs
            parts = (c, cl, cs)
        total = None
        for n in slices:
            u = load(v, SS + n, q)
            square = u * u
            f = force(u, square, pick_right(rolled(v, SS + n, q, SUB + 1, LANES - 1)),
                      pick_left(rolled(v, SS + n, q - 1, SUB + 1, 1)), parts)
            before = load(v, SS + n - 1, q)
            if n == 3:
                before = jnp.where(first, u, before)
            if n == 1:
                before = jnp.where(second, u, before)
            pull = f - 0.25 * (u - u * square)
            gap = before - u
            for m in range(M):
                if n == 1 and m < M - 1:
                    continue
                defect = gap + ROW_SUMS[m] * f
                new = newton(u, (3.0 * IMPLICIT[m]) * square, defect, before + ROW_SUMS[m] * pull, m)
                if n == 1:
                    v[E1, :, here] = new
                else:
                    keep(v, U1 + ((n - 2) * M + m) * 3, q, new)
                if n >= 3 and counted:
                    total = defect * defect if total is None else total + defect * defect
        if total is not None:
            add_up(0, first_col + q, total)

    def later_sweep(v, first_col, k, q, slices, counted):
        here = cols(q, SUB)
        parts = (load(v, CP, q), load(v, CL, q), load(v, CS, q))
        total = None
        for n in slices:
            at = U1 + (n - 2) * M * 3 if k == 1 else U2 + (n - 3) * M * 3
            us, squares, forces = [], [], []
            for m in range(M):
                u = load(v, at + 3 * m, q)
                square = u * u
                right = pick_right(load(v, at + 3 * m + 1, q, SUB + 1))
                left = pick_left(load(v, at + 3 * m + 2, q - 1, SUB + 1))
                us.append(u)
                squares.append(square)
                forces.append(force(u, square, right, left, parts))
            if n == 2:
                before = load(v, E1, q)
            elif n == 3:
                before = load(v, U1 + (M - 1) * 3 if k == 1 else E2, q)
                before = jnp.where(first, load(v, SS + 3, q), before)
            else:
                before = load(v, at - 3, q)
            for m in range(M):
                if n == 2 and m < M - 1:
                    continue
                base = before
                for j in range(M):
                    base = base + WEIGHTS[m][j] * forces[j]
                a = IMPLICIT[m]
                defect = base - us[m]
                scaled = a * squares[m]
                target = defect + us[m] * ((1.0 - a) + scaled)
                new = newton(us[m], 3.0 * scaled, defect, target, m)
                if n == 2:
                    v[E2, :, here] = new
                elif k == 1:
                    keep(v, U2 + ((n - 3) * M + m) * 3, q, new)
                else:
                    v[OUT + (n - 3) * M + m, :, here] = new
                if n >= 3 and counted:
                    total = defect * defect if total is None else total + defect * defect
        if total is not None:
            add_up(k, first_col + q, total)

    def window(step):
        return arena.at[:, :, cols(step * TILE, TILE + 6)], step * TILE

    def main_part(step, counted=True):
        v, at = window(step)
        for g in range(0, TILE, SUB):
            start_sweep(v, at, 3 + g, (4, 3, 2), counted)
        for g in range(0, TILE, SUB):
            later_sweep(v, at, 1, 2 + g, (4, 3), counted)
        for g in range(0, TILE, SUB):
            later_sweep(v, at, 2, 1 + g, (4,), counted)

    def lagging_part(step, counted=True):
        v, at = window(step)
        for g in range(0, TILE, SUB):
            start_sweep(v, at, 3 + g, (1,), counted)
        for g in range(0, TILE, SUB):
            later_sweep(v, at, 1, 2 + g, (2,), counted)
        for g in range(0, TILE, SUB):
            later_sweep(v, at, 2, 1 + g, (3,), counted)

    step_of = (1, M - 1)

    def send_out(which, i, part=0):
        place = cols(core * half + TILE * i + (half - MIX if part else 0), TILE)
        dst = out_ref.at[0, 0, rows[part], place]

        def out(away):
            to_node = lax.rem(node + away, M)
            src = arena.at[OUT + which * M + to_node, :, cols((second_pad if part else PAD) + TILE * i, TILE)]
            to = remote(src, dst, osend.at[which, away], orecv.at[core, away], dev(chip, which), to_node)
            if away:
                to.start()
            else:
                pl.when(core != which)(to.start)
                pl.when(core == which)(pltpu.make_async_copy(src, dst, osend.at[which, 0]).start)

        out(step_of[which])
        if not part:
            @pl.when(i < (half - MIX) // TILE)
            def _():
                out(2)
                out(M - step_of[which])
        out(0)

    wait_set(0)

    @pl.when(far_middle)
    def _():
        second_leg(0)
        pl.loop(1, AHEAD)(lambda a: second_leg(a))

    wait_far_set(0)

    @pl.loop(0, tiles + 1 + LAG)
    def _(step):
        @pl.when(far_middle)
        def _():
            a = step + AHEAD
            each_set(a, second_leg)

            @pl.when(a == main_sets)
            def _():
                second_leg(main_sets)

            @pl.when(jnp.logical_and(a > main_sets, a < sets - 1))
            def _():
                second_leg(a, 1)

        @pl.when(step <= tiles)
        def _():
            i = step - 1
            each_set(step + 1, wait_set)
            main_part(step)
            pl.when(i >= 0)(lambda: send_out(1, i))

        @pl.when(step >= LAG)
        def _():
            i = step - 1 - LAG
            each_set(i + 2, wait_far_set)
            lagging_part(step - LAG)
            pl.when(i >= 0)(lambda: send_out(0, i))

    @pl.when(far_middle)
    def _():
        pl.loop(tiles + 1 + LAG + AHEAD, sets - 1)(lambda a: second_leg(a, 1))
        second_leg(sets - 1)

    row = lax.broadcasted_iota(jnp.int32, (ROWS, LANES), 0)
    column = lax.broadcasted_iota(jnp.int32, (ROWS, LANES), 1)
    place = column == node * ROWS + row
    sums = jnp.zeros((ROWS, LANES), jnp.float32)
    for k in range(SWEEPS):
        spread = jnp.where(place, jnp.sum(acc[k], axis=1, keepdims=True), 0.0)
        sums = jnp.where(row == k, jnp.sum(spread, axis=0, keepdims=True), sums)

    def swap(store, mine, value, peers, send, recv):
        store[mine] = value
        flows = [
            remote(store.at[mine], store.at[mine], send.at[by], recv.at[by], to_tm, to_node)
            for by, (to_tm, to_node) in enumerate(peers)
        ]
        for c in flows:
            c.start()
        return flows

    pl.semaphore_wait(met, ny - 1)
    others = [lax.rem(ypos + by, ny) * nz + lax.rem(zpos + bz, nz) for by in range(ny) for bz in range(nz) if by or bz]
    flows = swap(st1, chip, sums, [(dev(c, core), node) for c in others], s1s, s1r)

    wait_set(main_sets)
    wait_far_set(main_sets)

    @pl.loop(0, MIX // TILE + 1)
    def _(step):
        a = main_sets + 1 + step

        def arrive(a):
            wait_set(a, 1)
            wait_far_set(a, 1)

        pl.when(a < sets - 1)(lambda: arrive(a))
        pl.when(a == sets - 1)(lambda: arrive(sets - 1))
        main_part(second_window + step, False)
        lagging_part(second_window + step, False)

        @pl.when(step > 0)
        def _():
            send_out(1, step - 1, 1)
            send_out(0, step - 1, 1)

    for c in flows:
        c.wait()
    sums = st1[0]
    for slot in range(1, chips):
        sums = sums + st1[slot]
    me = node * CORES + core
    peers = [lax.rem(me + by, M * CORES) for by in range(1, M * CORES)]
    flows = swap(st2, me, sums, [(dev(chip, lax.rem(p, CORES)), lax.div(p, CORES)) for p in peers], s2s, s2r)
    for c in flows:
        c.wait()
    sums = st2[0]
    for slot in range(1, M * CORES):
        sums = sums + st2[slot]
    sums_ref[...] = sums

    def ended(flow, count):
        view = own.at[0, :, cols(0, count)]
        pltpu.make_async_copy(view, view, zsend.at[flow]).wait()

    taken = half + MIX + 4
    ended(4, taken)

    @pl.when(has_next)
    def _():
        ended(0, taken)
        ended(1, taken)

    @pl.when(far_source)
    def _():
        for which in range(CORES):
            ended(2 + which, taken)

    @pl.when(far_middle)
    def _():
        for which in range(CORES):
            ended(5 + which, taken)

    def drained(sem, count):
        view = arena.at[OUT, :, cols(0, count)]
        pltpu.make_async_copy(view, view, sem).wait()

    more, less = half + MIX, half - MIX
    for which in range(CORES):
        for away in range(M):
            drained(osend.at[which, away], more if away in (0, step_of[which]) else less)
        drained(orecv.at[which, 2], less)
        for away in (1, M - 1):
            up = core == 0 if away == 1 else core == 1
            pl.when(up)(functools.partial(drained, orecv.at[which, away], more))
            pl.when(jnp.logical_not(up))(functools.partial(drained, orecv.at[which, away], less))
    drained(orecv.at[1 - core, 0], more)


def finish(mean_count, made_ref, sums_ref, out_ref, log_ref, row, sem):
    systems = made_ref.shape[2]
    flows = []
    for block in range(systems // ROWS):
        rows = pl.ds(block * ROWS, ROWS)
        flows.append(pltpu.make_async_copy(made_ref.at[0, 0, rows], out_ref.at[0, 0, rows], sem.at[block]))
    for c in flows:
        c.start()
    row[...] = jnp.log(log_floor + sums_ref[...] / mean_count)[:SWEEPS, :systems]
    last = pltpu.make_async_copy(row, log_ref, sem.at[systems // ROWS])
    last.start()
    for c in flows:
        c.wait()
    last.wait()


def body(sizes, slice_starts, coupling):
    systems, cells = coupling.shape
    ny, nz = sizes
    half = cells // LANES // CORES
    tiles = half // TILE
    sets = tiles + 4 + MIX // TILE
    span = (tiles + 3) * TILE + MIX + TILE + 6
    mean_count = float(ny * nz * CORES * M * cells)
    flat = lambda *lead: pltpu.VMEM(lead + (ROWS, span * LANES), jnp.float32)
    dma = pltpu.SemaphoreType.DMA
    any_spec = pl.BlockSpec(memory_space=pl.ANY)
    out = jax.ShapeDtypeStruct((1, 1, systems, cells), jnp.float32)
    made, sums = pl.pallas_call(
        functools.partial(kernel, (ny, nz, cells)),
        out_shape=(out, jax.ShapeDtypeStruct((ROWS, LANES), jnp.float32)),
        in_specs=[pl.BlockSpec(memory_space=pltpu.HBM)] * 2,
        out_specs=(any_spec, pl.BlockSpec(memory_space=pltpu.VMEM)),
        scratch_shapes=[
            pltpu.VMEM((2, ROWS, cells), jnp.float32), flat(CORES), flat(PLACES),
            pltpu.VMEM((SWEEPS, ROWS, LANES), jnp.float32),
            pltpu.VMEM((ny * nz, ROWS, LANES), jnp.float32),
            pltpu.VMEM((M * CORES, ROWS, LANES), jnp.float32),
            dma((2,)), dma((sets,)), dma((5, sets)), dma((CORES, sets)), dma((7,)),
            dma((CORES, M)), dma((CORES, M)),
            dma((ny * nz,)), dma((ny * nz,)), dma((M * CORES,)), dma((M * CORES,)),
            pltpu.SemaphoreType.REGULAR,
        ],
        compiler_params=pltpu.CompilerParams(
            collective_id=0, has_side_effects=True, vmem_limit_bytes=51 * 2**20
        ),
        name="sdc",
    )(slice_starts, coupling)
    return pl.pallas_call(
        functools.partial(finish, mean_count),
        out_shape=(out, jax.ShapeDtypeStruct((SWEEPS, systems), jnp.float32)),
        in_specs=[any_spec, pl.BlockSpec(memory_space=pltpu.VMEM)],
        out_specs=(pl.BlockSpec(memory_space=pltpu.HBM),) * 2,
        scratch_shapes=[pltpu.VMEM((SWEEPS, systems), jnp.float32), dma((systems // ROWS + 1,))],
        compiler_params=pltpu.CompilerParams(vmem_limit_bytes=2**20),
        name="finish",
    )(made, sums)


def solution(mesh):
    chips = mesh.shape["tm"] // CORES
    ny = 4
    return jax.shard_map(
        functools.partial(body, (ny, chips // ny)),
        mesh=mesh,
        in_specs=(P("tm", None, None), P()),
        out_specs=(P("tm", "node", None, None), P()),
        check_vma=False,
    )
```
